512 devices in a mesh: groups: 2 (over y), seg: 32 (over z, core), bin: 8 (over x).
Axes of the slice: x: 8, y: 2, z: 16, core: 2. Of those that a mesh axis runs over, the one named last changes fastest.
The devices are a block of a 8x8x16 slice.
Arguments:
- start_factors: float32 [32768, 128], P(('groups', 'seg', 'bin')), parts along dimension 0, may hold values from -6 to 6
- bin_factors: bfloat16 [16384, 128], P(('groups', 'bin')), parts along dimension 0, may hold values from -0.5 to 0.5
- tile_speed: bfloat16 [64, 8, 12, 128, 128], P(('groups', 'seg'), 'bin'), parts along dimension 0, may hold values from -6 to 6
- tile_weight: bfloat16 [64, 8, 12, 128, 128], P(('groups', 'seg'), 'bin'), parts along dimension 0, may hold values from 0.099609375 to 2
- tile_cells: int32 [64, 8, 12, 2], P(('groups', 'seg'), 'bin'), parts along dimension 0, may hold values from 0 to 7, as said below
- tile_count: int32 [64, 8], P(('groups', 'seg'), 'bin'), parts along dimension 0, may hold values from 1 to 12, as said below
- inner_pairs: int32 [64, 8, 2, 2], P(('groups', 'seg'), 'bin'), parts along dimension 0, may hold values from 0 to 3, as said below
- inner_weight: float32 [64, 8, 2, 128, 128], P(('groups', 'seg'), 'bin'), parts along dimension 0, may hold values from 0 to 0.00390625
- face_rows: int32 [64, 8, 2, 256], P(('groups', 'seg'), 'bin'), parts along dimension 0, may hold values from 0 to 511, as said below
- face_count: int32 [64, 8, 2], P(('groups', 'seg'), 'bin'), parts along dimension 0, may hold values from 128 to 256, as said below
- face_weight: float32 [64, 8, 256, 256], P(('groups', 'seg'), 'bin'), parts along dimension 0, may hold values from 0 to 0.00390625
Outputs:
- solution_factors: float32 [32768, 128], P(('groups', 'seg', 'bin')), parts along dimension 0
- residual: float32 [32768, 128], P(('groups', 'seg', 'bin')), parts along dimension 0
The draws below stay inside these ranges and needn't reach their ends.
There are 2 independent parts, one for each index of `groups`. The reference program is written for one: setup_inputs(seed, part) draws one part's arguments, and reference() takes and returns one part's arrays. A program takes and returns all parts, laid end to end along the dimension named above; each array names one. Nothing has to cross between parts.
Inputs may be any that keep to these rules, and one draw needn't show every extreme that they name: `tile_cells`: the 12 slots of one device name different pairs; the first entry is a segment block of the partition, the second a bin block of the device's bins. `tile_count`: some device of every draw has all 12 slots live. `inner_pairs`: the two blocks of a pair differ; both are segment blocks of the partition. `face_rows`: row numbers within the partition, different within each face list. `face_count`: some face list of every draw has all 256 rows live.
All inputs are finite; a program needn't handle non-finite values.
Results may differ from the reference program's by a relative error of at most 0.0024.
Values sent between devices are 32-bit elements; how exact they have to be, the bound alone decides.
A program may use at most 64 MiB of HBM per device.

```python
import jax
import jax.numpy as jnp
from jax import lax

TILE = 128
R = 128
SEGBLK_DEV = 4
BINBLK_DEV = 8
HR = 256
ITERS = 2
NT_DEV = 12
NI = 2
SEGS = 16384
BINS = 8192
N_SEG = 32
N_BIN = 8


def draw_tile_count(key, part):
    key_one, key_two, key_three = jax.random.split(key, 3)
    first = jax.random.randint(key_one, (N_SEG * N_BIN,), 0, NT_DEV)
    second = jax.random.randint(key_two, (N_SEG * N_BIN,), 0, NT_DEV)
    counts = 1 + first * second // NT_DEV
    chosen = jax.random.randint(key_three, (), 0, N_SEG * N_BIN)
    counts = jnp.where(jnp.arange(N_SEG * N_BIN) == chosen, NT_DEV, counts)
    return counts.reshape(N_SEG, N_BIN).astype(jnp.int32)


def draw_tile_cells(key, part):
    key_list = jax.random.split(key, N_SEG * N_BIN)
    shuffled = jax.vmap(lambda single: jax.random.permutation(single, SEGBLK_DEV * BINBLK_DEV)[:NT_DEV])(key_list)
    cells = jnp.stack([shuffled // BINBLK_DEV, shuffled % BINBLK_DEV], axis=-1)
    return cells.reshape(N_SEG, N_BIN, NT_DEV, 2).astype(jnp.int32)


def draw_inner_pairs(key, part):
    key_one, key_two = jax.random.split(key)
    first = jax.random.randint(key_one, (N_SEG, N_BIN, NI), 0, SEGBLK_DEV)
    offset = jax.random.randint(key_two, (N_SEG, N_BIN, NI), 1, SEGBLK_DEV)
    second = (first + offset) % SEGBLK_DEV
    return jnp.stack([first, second], axis=-1).astype(jnp.int32)


def draw_face_rows(key, part):
    key_list = jax.random.split(key, N_SEG * N_BIN * 2)
    shuffled = jax.vmap(lambda single: jax.random.permutation(single, TILE * SEGBLK_DEV)[:HR])(key_list)
    return shuffled.reshape(N_SEG, N_BIN, 2, HR).astype(jnp.int32)


def draw_face_count(key, part):
    key_one, key_two = jax.random.split(key)
    halfway = HR // 2
    counts = halfway + jax.random.randint(key_one, (N_SEG * N_BIN * 2,), 0, HR - halfway + 1)
    chosen = jax.random.randint(key_two, (), 0, N_SEG * N_BIN * 2)
    counts = jnp.where(jnp.arange(N_SEG * N_BIN * 2) == chosen, HR, counts)
    return counts.reshape(N_SEG, N_BIN, 2).astype(jnp.int32)


def steps_of(own_key, dims, pieces, least, largest):
    def one(dim, parts):
        steps = jax.random.uniform(jax.random.fold_in(jax.random.fold_in(own_key, 6), dim), (parts,), jnp.float32, least / len(pieces), largest / len(pieces))
        return jnp.repeat(jnp.exp(steps), dims[dim] // parts).reshape((-1,) + (1,) * (len(dims) - dim - 1))

    gain = one(*pieces[0])
    for cut in pieces[1:]:
        gain = gain * one(*cut)
    return gain


def noise(own_key, shape, spread, most, cuts=(), kind=jnp.bfloat16):
    array = spread * jax.random.normal(own_key, shape, jnp.float32)
    if cuts:
        array = array * steps_of(own_key, shape, cuts, -0.22, 0.18)
    return jnp.clip(array, -most, most).astype(kind)


def setup_inputs(seed: int = 0, part: int = 0) -> dict:
    keys = jax.random.split(jax.random.key(seed), 12)
    part_splits = jax.random.split(jax.random.fold_in(keys[11], part), 12)
    return {
        "start_factors": noise(part_splits[0], (SEGS, R), 1.0, 6.0, ((0, 256),), jnp.float32),
        "bin_factors": noise(part_splits[1], (BINS, R), R ** -0.5, 0.5, ((0, 8),)),
        "tile_speed": noise(part_splits[2], (N_SEG, N_BIN, NT_DEV, TILE, TILE), 1.0, 6.0, ((0, 32), (1, 8))),
        "tile_weight": jnp.clip(0.099609375 + 1.9003906 * jax.random.uniform(part_splits[3], (N_SEG, N_BIN, NT_DEV, TILE, TILE), jnp.float32) ** steps_of(part_splits[3], (N_SEG, N_BIN, NT_DEV, TILE, TILE), ((0, 32), (1, 8)), -0.2, 0.2), 0.099609375, 2.0).astype(jnp.bfloat16),
        "tile_cells": draw_tile_cells(jax.random.fold_in(jax.random.fold_in(keys[11], part), 71), part),
        "tile_count": draw_tile_count(jax.random.fold_in(jax.random.fold_in(keys[11], part), 71), part),
        "inner_pairs": draw_inner_pairs(jax.random.fold_in(jax.random.fold_in(keys[11], part), 71), part),
        "inner_weight": jnp.clip(0.00390625 * jax.random.uniform(part_splits[7], (N_SEG, N_BIN, NI, TILE, TILE), jnp.float32) ** steps_of(part_splits[7], (N_SEG, N_BIN, NI, TILE, TILE), ((0, 32), (1, 8)), -0.2, 0.2), 0.0, 0.00390625),
        "face_rows": draw_face_rows(jax.random.fold_in(jax.random.fold_in(keys[11], part), 71), part),
        "face_count": draw_face_count(jax.random.fold_in(jax.random.fold_in(keys[11], part), 71), part),
        "face_weight": jnp.clip(0.00390625 * jax.random.uniform(part_splits[10], (N_SEG, N_BIN, HR, HR), jnp.float32) ** steps_of(part_splits[10], (N_SEG, N_BIN, HR, HR), ((0, 32), (1, 8)), -0.2, 0.2), 0.0, 0.00390625),
    }


highest = lax.Precision.HIGHEST
ridge_weight = 0.5


def tile_image(factors, bin_factors, tile_cells, tile_count, tile_weight):
    blocks_all = factors.reshape(N_SEG, SEGBLK_DEV, TILE, R)
    bins_all = bin_factors.astype(jnp.float32).reshape(N_BIN, BINBLK_DEV, TILE, R)
    bin_index = jnp.arange(N_BIN, dtype=jnp.int32)[:, None]
    slot_index = jnp.arange(NT_DEV, dtype=jnp.int32)[None, :]

    def one_part(packed):
        blocks, cells, counts, weights = packed
        picked = blocks[cells[:, :, 0]]
        chosen = bins_all[bin_index, cells[:, :, 1]]
        live_tiles = (slot_index < counts[:, None]).astype(jnp.float32)
        tile_gain = weights.astype(jnp.float32) * live_tiles[:, :, None, None]
        scores = jnp.einsum("tkir,tkjr->tkij", picked, chosen, precision=highest) * tile_gain
        pulled = jnp.einsum("tkij,tkjr->tkir", scores, chosen, precision=highest)
        return jnp.zeros((SEGBLK_DEV, TILE, R), jnp.float32).at[cells[:, :, 0]].add(pulled)

    return lax.map(one_part, (blocks_all, tile_cells, tile_count, tile_weight)).reshape(-1, R)


def right_side(bin_factors, tile_speed, tile_weight, tile_cells, tile_count):
    bins_all = bin_factors.reshape(N_BIN, BINBLK_DEV, TILE, R)
    bin_index = jnp.arange(N_BIN, dtype=jnp.int32)[:, None]
    slot_index = jnp.arange(NT_DEV, dtype=jnp.int32)[None, :]

    def one_part(packed):
        speeds, weights, cells, counts = packed
        chosen = bins_all[bin_index, cells[:, :, 1]].astype(jnp.float32)
        weighted = (weights.astype(jnp.float32) * speeds.astype(jnp.float32)).astype(jnp.bfloat16)
        live_tiles = (slot_index < counts[:, None]).astype(jnp.float32)
        terms = jnp.einsum("tkij,tkjr->tkir", weighted.astype(jnp.float32), chosen, precision=highest)
        terms = terms * live_tiles[:, :, None, None]
        return jnp.zeros((SEGBLK_DEV, TILE, R), jnp.float32).at[cells[:, :, 0]].add(terms)

    return lax.map(one_part, (tile_speed, tile_weight, tile_cells, tile_count)).reshape(-1, R)


def inner_image(factors, inner_pairs, inner_weight):
    blocks = factors.reshape(N_SEG, SEGBLK_DEV, TILE, R)
    part_index = jnp.arange(N_SEG, dtype=jnp.int32)[:, None, None]
    left = blocks[part_index, inner_pairs[..., 0]]
    right = blocks[part_index, inner_pairs[..., 1]]
    to_left = inner_weight.sum(4)[..., None] * left - jnp.einsum("stkij,stkjr->stkir", inner_weight, right, precision=highest)
    to_right = inner_weight.sum(3)[..., None] * right - jnp.einsum("stkij,stkir->stkjr", inner_weight, left, precision=highest)
    summed = jnp.zeros_like(blocks).at[part_index, inner_pairs[..., 0]].add(to_left)
    summed = summed.at[part_index, inner_pairs[..., 1]].add(to_right)
    return summed.reshape(-1, R)


def face_image(factors, face_rows, face_count, face_weight):
    part_rows = factors.reshape(N_SEG, SEGBLK_DEV * TILE, R)
    part_index = jnp.arange(N_SEG, dtype=jnp.int32)[:, None, None]
    slots = jnp.arange(HR, dtype=jnp.int32)[None, None, :]
    rows_low = face_rows[:, :, 0]
    rows_up = face_rows[:, :, 1]
    mask_low = (slots < face_count[:, :, 0:1]).astype(jnp.float32)
    mask_up = (slots < face_count[:, :, 1:2]).astype(jnp.float32)
    own_face = part_rows[part_index, rows_low] * mask_low[..., None]
    upper_face = part_rows[part_index, rows_up] * mask_up[..., None]
    lower_face = jnp.concatenate([jnp.zeros_like(upper_face[:1]), upper_face[:-1]], axis=0)
    lower_mask = jnp.concatenate([jnp.zeros_like(mask_up[:1]), mask_up[:-1]], axis=0)
    coupling = face_weight * mask_low[..., :, None] * lower_mask[..., None, :]
    own_term = coupling.sum(3)[..., None] * own_face - jnp.einsum("stij,stjr->stir", coupling, lower_face, precision=highest)
    answer = coupling.sum(2)[..., None] * lower_face - jnp.einsum("stij,stir->stjr", coupling, own_face, precision=highest)
    returned = jnp.concatenate([answer[1:], jnp.zeros_like(answer[:1])], axis=0)
    summed = jnp.zeros_like(part_rows).at[part_index, rows_low].add(own_term)
    summed = summed.at[part_index, rows_up].add(returned)
    return summed.reshape(-1, R)


def reference(start_factors, bin_factors, tile_speed, tile_weight, tile_cells, tile_count, inner_pairs, inner_weight, face_rows, face_count, face_weight):
    def operator(field):
        summed = tile_image(field, bin_factors, tile_cells, tile_count, tile_weight)
        summed = summed + inner_image(field, inner_pairs, inner_weight)
        summed = summed + face_image(field, face_rows, face_count, face_weight)
        return summed + ridge_weight * field

    rhs_rows = right_side(bin_factors, tile_speed, tile_weight, tile_cells, tile_count)
    solution = start_factors
    residual = rhs_rows - operator(start_factors)
    direction = residual
    norm_now = jnp.sum(residual * residual)
    for iteration in range(ITERS):
        images = operator(direction)
        step_size = norm_now / jnp.sum(direction * images)
        solution = solution + step_size * direction
        residual = residual - step_size * images
        norm_next = jnp.sum(residual * residual)
        direction = residual + (norm_next / norm_now) * direction
        norm_now = norm_next
    return solution, residual
```

```python
import functools

import jax
import jax.numpy as jnp
from jax import lax
from jax.experimental import pallas as pl
from jax.experimental.pallas import tpu as pltpu
from jax.sharding import PartitionSpec as P

RIDGE = 0.5
APPLIES = 3
MESH = pl.DeviceIdType.MESH
f32 = jnp.float32
bf16 = jnp.bfloat16


def split(x):
    hi = x.astype(bf16)
    return hi, (x - hi.astype(f32)).astype(bf16)


def dot_nn(a, b):
    return jnp.dot(a, b, preferred_element_type=f32)


def dot_nt(a, b):
    return lax.dot_general(a, b, (((1,), (1,)), ((), ())), preferred_element_type=f32)


def kernel(
    n_bin,
    n_seg,
    x0_hbm,
    bins_hbm,
    speed_hbm,
    weight_hbm,
    cells_hbm,
    count_hbm,
    pairs_hbm,
    inner_hbm,
    rows_hbm,
    face_hbm,
    sol_ref,
    res_ref,
    field,
    below,
    above,
    part,
    landed,
    bins,
    speed,
    weight,
    cells,
    count,
    pairs,
    hits,
    inner,
    rows,
    rows_below,
    rows_above,
    face,
    face_above,
    gain,
    v_wide,
    v_tall,
    pulled,
    w_hi,
    w_lo,
    f_below,
    f_above,
    degree,
    rhs,
    wide,
    sums_mine,
    sums_seg,
    sums_far,
    sums_bin,
    load_sem,
    gather_send,
    gather_recv,
    below_send,
    below_recv,
    above_send,
    above_recv,
    scatter_send,
    scatter_recv,
    setup_send,
    setup_recv,
    sums_send,
    sums_recv,
):
    seg = lax.axis_index("seg")
    bin_ = lax.axis_index("bin")
    own = x0_hbm.shape[0]
    width = x0_hbm.shape[1]
    n_tiles = speed.shape[0]
    tile = speed.shape[1]
    n_inner = inner.shape[0]
    part_rows = own * n_bin
    n_blocks = part_rows // tile
    half = n_seg // 4
    seg_next = lax.rem(seg + 1, n_seg)
    seg_prev = lax.rem(seg + n_seg - 1, n_seg)

    def seg_at(offset):
        return lax.rem(seg + (offset + n_seg), n_seg)

    def bin_at(offset):
        return lax.rem(bin_ + offset, n_bin)

    def own_slice():
        return pl.ds(pl.multiple_of(bin_ * own, own), own)

    loads = []
    for at, (src, dst) in enumerate(
        (
            (x0_hbm, field.at[0, own_slice()]),
            (rows_hbm, rows),
            (cells_hbm, cells),
            (count_hbm, count),
            (pairs_hbm, pairs),
            (face_hbm, face),
            (bins_hbm, bins),
            (weight_hbm, weight),
            (speed_hbm, speed),
            (inner_hbm, inner),
        )
    ):
        copy = pltpu.make_async_copy(src, dst, load_sem.at[at])
        copy.start()
        loads.append(copy)

    barrier = pltpu.get_barrier_semaphore()
    seg_offsets = [d for d in range(-half, half + 1) if d != 0]
    for d in range(1, n_bin):
        pl.semaphore_signal(barrier, inc=1, device_id={"bin": bin_at(d)}, device_id_type=MESH)
    for d in seg_offsets:
        pl.semaphore_signal(barrier, inc=1, device_id={"seg": seg_at(d)}, device_id_type=MESH)

    def slots_and_gain():
        for load in loads[2:5] + loads[6:8]:
            load.wait()
        targets = [cells[k, 0] for k in range(n_tiles)]
        targets += [pairs[j // 2, j % 2] for j in range(2 * n_inner)]
        for item, target in enumerate(targets):
            for b in range(n_blocks):
                away = target - b
                hits[item, b] = (1 - jnp.minimum(away * away, 1)).astype(f32)
        for k in range(n_tiles):
            live = jnp.clip(count[0, 0] - k, 0, 1).astype(f32)
            gain[k] = weight[k].astype(f32) * live
            chosen = bins[cells[k, 1]]
            v_wide[k, :, :width] = chosen
            v_wide[k, :, width:] = chosen
            v_tall[k, :tile] = chosen
            v_tall[k, tile:] = chosen

    def add_up(items, block):
        total = None
        for ref_at, item in items:
            term = ref_at() * hits[item, block]
            total = term if total is None else total + term
        return total

    def right_side():
        loads[8].wait()
        for k in range(n_tiles):
            weighted = (weight[k].astype(f32) * speed[k].astype(f32)).astype(bf16)
            live = jnp.clip(count[0, 0] - k, 0, 1).astype(f32)
            pulled[k] = dot_nn(weighted, v_tall[k, :tile]) * live
        for b in range(n_blocks):
            items = [((lambda k=k: pulled[k]), k) for k in range(n_tiles)]
            rhs[b * tile : (b + 1) * tile] = add_up(items, b)

    def inner_setup():
        loads[9].wait()
        for j in range(n_inner):
            forward = inner[j]
            hi, lo = split(forward)
            w_hi[2 * j] = hi
            w_lo[2 * j] = lo
            back = forward.T
            hi, lo = split(back)
            w_hi[2 * j + 1] = hi
            w_lo[2 * j + 1] = lo
            pulled[2 * j] = jnp.broadcast_to(forward.sum(1, keepdims=True), (tile, width))
            pulled[2 * j + 1] = jnp.broadcast_to(back.sum(1, keepdims=True), (tile, width))

    def inner_degree(b):
        items = [((lambda j=j: pulled[j]), n_tiles + j) for j in range(2 * n_inner)]
        return add_up(items, b)

    def one_hot(row_ref, which):
        n_face = row_ref.shape[1]
        listed = jnp.broadcast_to(row_ref[which : which + 1, :], (part_rows, n_face))
        at = lax.broadcasted_iota(jnp.int32, (part_rows, n_face), 0)
        return jnp.where(listed == at, 1.0, 0.0).astype(bf16)

    def face_setup():
        low_own = one_hot(rows, 0)
        up_own = one_hot(rows, 1)
        up_below = one_hot(rows_below, 1)
        low_above = one_hot(rows_above, 0)
        down = jnp.where(seg > 0, 1.0, 0.0).astype(f32)
        up = jnp.where(seg < n_seg - 1, 1.0, 0.0).astype(f32)
        mine = split(face[...] * down)
        theirs = split(face_above[...] * up)
        degrees = jnp.zeros((part_rows, 1), f32)
        for p in range(2):
            picked = dot_nn(low_own, mine[p]).astype(bf16)
            whole = dot_nt(picked, up_below)
            f_below[p] = whole.astype(bf16)
            degrees = degrees + whole.sum(1, keepdims=True)
            picked = dot_nt(up_own, theirs[p]).astype(bf16)
            whole = dot_nt(picked, low_above)
            f_above[p] = whole.astype(bf16)
            degrees = degrees + whole.sum(1, keepdims=True)
        degree[...] = jnp.broadcast_to(degrees, (part_rows, width))
        for b in range(n_blocks):
            degree[b * tile : (b + 1) * tile] += inner_degree(b)

    def doubled(product):
        return product[:, :width] + product[:, width:]

    def local_terms(step):
        hi, lo = split(field[step])
        for b in range(n_blocks):
            wide[b, :, :width] = hi[b * tile : (b + 1) * tile]
            wide[b, :, width:] = lo[b * tile : (b + 1) * tile]
        for k in range(n_tiles):
            picked = wide[cells[k, 0]]
            scores = dot_nt(picked, v_wide[k]) * gain[k]
            hi, lo = split(scores)
            pulled[k] = dot_nn(jnp.concatenate([hi, lo], axis=1), v_tall[k])
        for j in range(n_inner):
            for way in range(2):
                picked = wide[pairs[j, 1 - way]]
                product = doubled(dot_nn(w_hi[2 * j + way], picked))
                product = product + dot_nn(w_lo[2 * j + way], picked[:, :width])
                pulled[n_tiles + 2 * j + way] = -product

    def face_terms(step):
        total = None
        for matrix, source in ((f_below, below), (f_above, above)):
            hi, lo = split(source[step])
            both = jnp.concatenate([hi, lo], axis=1)
            product = doubled(dot_nn(matrix[0], both)) + dot_nn(matrix[1], hi)
            total = product if total is None else total + product
        return total

    def join(step, faces):
        items = [((lambda k=k: pulled[k]), k) for k in range(n_tiles)]
        for j in range(2 * n_inner):
            items.append(((lambda j=j: pulled[n_tiles + j]), n_tiles + j))
        for b in range(n_blocks):
            at = slice(b * tile, (b + 1) * tile)
            value = add_up(items, b) + degree[at] * field[step, at] - faces[at]
            part[step, at] = rhs[at] - value if step == 0 else value

    order = sorted(range(1, n_bin), key=lambda d: -min(d, n_bin - d))

    def to_bin(src, dst, send, recv, d):
        return pltpu.make_async_remote_copy(
            src_ref=src, dst_ref=dst, send_sem=send, recv_sem=recv,
            device_id={"bin": bin_at(d)}, device_id_type=MESH,
        )

    def to_seg(src, dst, send, recv, where):
        return pltpu.make_async_remote_copy(
            src_ref=src, dst_ref=dst, send_sem=send, recv_sem=recv,
            device_id={"seg": where}, device_id_type=MESH,
        )

    def forward(step, source):
        rows_at = pl.ds(pl.multiple_of(source * own, own), own)
        block = field.at[step, rows_at]
        to_seg(block, below.at[step, rows_at], below_send.at[step], below_recv.at[step], seg_next).start()
        to_seg(block, above.at[step, rows_at], above_send.at[step], above_recv.at[step], seg_prev).start()

    def gather_start(step):
        mine = field.at[step, own_slice()]
        for d in order:
            to_bin(mine, mine, gather_send.at[step], gather_recv.at[step, d], d).start()
        forward(step, bin_)

    def gather_finish(step):
        for d in reversed(order):
            source = lax.rem(bin_ + (n_bin - d), n_bin)
            rows_at = pl.ds(pl.multiple_of(source * own, own), own)
            block = field.at[step, rows_at]
            pltpu.make_async_copy(block, block, gather_recv.at[step, d]).wait()
            forward(step, source)

    def faces_finish(step):
        pltpu.make_async_copy(below.at[step], below.at[step], below_recv.at[step]).wait()
        pltpu.make_async_copy(above.at[step], above.at[step], above_recv.at[step]).wait()

    def scatter_start(step):
        for d in order:
            target = bin_at(d)
            block = part.at[step, pl.ds(pl.multiple_of(target * own, own), own)]
            to_bin(block, landed.at[step, d - 1], scatter_send.at[step], scatter_recv.at[step], d).start()

    def scatter_finish(step):
        pltpu.make_async_copy(landed.at[step], landed.at[step], scatter_recv.at[step]).wait()
        total = part[step, own_slice()]
        for d in range(n_bin - 1):
            total = total + landed[step, d]
        return total

    window = [e for e in range(-half + 1, half + 1) if e != 0]

    def two_sums(first, second):
        lanes = lax.broadcasted_iota(jnp.int32, (1, width), 1)
        first = first.sum(0, keepdims=True)
        second = second.sum(0, keepdims=True)
        first = first + pltpu.roll(first, width // 2, 1)
        second = second + pltpu.roll(second, width // 2, 1)
        return jnp.where(lanes < width // 2, first, second)

    def sums_start(turn, value):
        sums_mine[turn, 0] = value
        for at, e in enumerate(window):
            to_seg(sums_mine.at[turn, 0], sums_seg.at[turn, at], sums_send.at[turn, 0], sums_recv.at[turn, 0], seg_at(e)).start()

    def sums_second(turn):
        pltpu.make_async_copy(sums_seg.at[turn], sums_seg.at[turn], sums_recv.at[turn, 0]).wait()
        total = sums_mine[turn, 0]
        for at in range(len(window)):
            total = total + sums_seg[turn, at]
        sums_mine[turn, 1] = total
        for at, e in enumerate((-half, half)):
            to_seg(sums_mine.at[turn, 1], sums_far.at[turn, at], sums_send.at[turn, 1], sums_recv.at[turn, 1], seg_at(e)).start()

    def sums_third(turn):
        pltpu.make_async_copy(sums_far.at[turn], sums_far.at[turn], sums_recv.at[turn, 1]).wait()
        total = sums_far[turn, 0] + sums_far[turn, 1]
        sums_mine[turn, 2] = total
        for d in order:
            to_bin(sums_mine.at[turn, 2], sums_bin.at[turn, d - 1], sums_send.at[turn, 2], sums_recv.at[turn, 2], d).start()

    def sums_finish(turn):
        pltpu.make_async_copy(sums_bin.at[turn], sums_bin.at[turn], sums_recv.at[turn, 2]).wait()
        total = sums_mine[turn, 2]
        for d in range(n_bin - 1):
            total = total + sums_bin[turn, d]
        lanes = lax.broadcasted_iota(jnp.int32, (1, width), 1)
        first = jnp.sum(jnp.where(lanes < width // 2, total, 0.0), axis=1, keepdims=True)
        second = jnp.sum(jnp.where(lanes < width // 2, 0.0, total), axis=1, keepdims=True)
        return first, second

    slots_and_gain()
    loads[0].wait()
    loads[1].wait()
    loads[5].wait()
    pl.semaphore_wait(barrier, n_bin - 1 + len(seg_offsets))
    to_seg(rows, rows_below, setup_send.at[0], setup_recv.at[0], seg_next).start()
    to_seg(rows, rows_above, setup_send.at[1], setup_recv.at[1], seg_prev).start()
    gather_start(0)
    to_seg(face, face_above, setup_send.at[2], setup_recv.at[2], seg_prev).start()
    right_side()
    inner_setup()
    gather_finish(0)
    pltpu.make_async_copy(rows, rows_below, setup_recv.at[0]).wait()
    pltpu.make_async_copy(rows, rows_above, setup_recv.at[1]).wait()
    pltpu.make_async_copy(face, face_above, setup_recv.at[2]).wait()
    face_setup()
    local_terms(0)
    faces_finish(0)
    join(0, face_terms(0))
    scatter_start(0)
    start = field[0, own_slice()]
    residual = scatter_finish(0) - RIDGE * start
    field[1, own_slice()] = residual

    gather_start(1)
    gather_finish(1)
    local_terms(1)
    faces_finish(1)
    join(1, face_terms(1))
    square = residual * residual
    sums_start(0, two_sums(square, field[1] * part[1]))
    scatter_start(1)
    sums_second(0)
    image = scatter_finish(1) + RIDGE * field[1, own_slice()]
    field[2, own_slice()] = image
    gather_start(2)
    sums_third(0)

    gather_finish(2)
    local_terms(2)
    faces_finish(2)
    join(2, face_terms(2))
    norm, product = sums_finish(0)
    product = product + RIDGE * norm
    step_one = norm / product
    residual = field[1, own_slice()]
    image = field[2, own_slice()]
    later = residual - step_one * image
    whole = field[1] - step_one * field[2]
    whole_image = part[1] - step_one * part[2]
    sums_start(1, two_sums(later * later, whole * whole_image))
    scatter_start(2)
    sums_second(1)
    sums_third(1)
    image_two = scatter_finish(2) + RIDGE * field[2, own_slice()]
    norm_next, product_next = sums_finish(1)
    product_next = product_next + RIDGE * norm_next
    beta = norm_next / norm
    step_two = norm_next / (product_next - beta * norm_next / step_one)
    residual = field[1, own_slice()]
    image = field[2, own_slice()]
    later = residual - step_one * image
    later_image = image - step_one * image_two
    direction = later + beta * residual
    along = later_image + beta * image
    sol_ref[...] = field[0, own_slice()] + step_one * residual + step_two * direction
    res_ref[...] = later - step_two * along

    pltpu.make_async_copy(rows, rows, setup_send.at[0]).wait()
    pltpu.make_async_copy(rows, rows, setup_send.at[1]).wait()
    pltpu.make_async_copy(face, face, setup_send.at[2]).wait()
    for step in range(APPLIES):
        pltpu.make_async_copy(landed.at[step], landed.at[step], gather_send.at[step]).wait()
        pltpu.make_async_copy(landed.at[step], landed.at[step], scatter_send.at[step]).wait()
        pltpu.make_async_copy(below.at[step], below.at[step], below_send.at[step]).wait()
        pltpu.make_async_copy(above.at[step], above.at[step], above_send.at[step]).wait()
    for turn in range(2):
        pltpu.make_async_copy(sums_seg.at[turn], sums_seg.at[turn], sums_send.at[turn, 0]).wait()
        pltpu.make_async_copy(sums_far.at[turn], sums_far.at[turn], sums_send.at[turn, 1]).wait()
        pltpu.make_async_copy(sums_bin.at[turn], sums_bin.at[turn], sums_send.at[turn, 2]).wait()


def shards(
    n_bin,
    n_seg,
    start_factors,
    bin_factors,
    tile_speed,
    tile_weight,
    tile_cells,
    tile_count,
    inner_pairs,
    inner_weight,
    face_rows,
    face_count,
    face_weight,
):
    own, width = start_factors.shape
    n_tiles, tile = tile_speed.shape[2:4]
    n_inner = inner_weight.shape[2]
    n_face = face_rows.shape[3]
    part_rows = own * n_bin
    slots = jnp.arange(n_face, dtype=jnp.int32)
    listed = jnp.where(slots[None, :] < face_count[0, 0][:, None], face_rows[0, 0], -1)
    half = n_seg // 4
    window = 2 * half - 1
    any_ = pl.BlockSpec(memory_space=pl.ANY)
    vmem = pl.BlockSpec(memory_space=pltpu.VMEM)
    dma = pltpu.SemaphoreType.DMA
    out = jax.ShapeDtypeStruct((own, width), f32)
    call = pl.pallas_call(
        functools.partial(kernel, n_bin, n_seg),
        out_shape=(out, out),
        in_specs=[any_] * 10,
        out_specs=(vmem, vmem),
        scratch_shapes=[
            pltpu.VMEM((APPLIES, part_rows, width), f32),
            pltpu.VMEM((APPLIES, part_rows, width), f32),
            pltpu.VMEM((APPLIES, part_rows, width), f32),
            pltpu.VMEM((APPLIES, part_rows, width), f32),
            pltpu.VMEM((APPLIES, n_bin - 1, own, width), f32),
            pltpu.VMEM((bin_factors.shape[0] // tile, tile, width), bf16),
            pltpu.VMEM((n_tiles, tile, tile), bf16),
            pltpu.VMEM((n_tiles, tile, tile), bf16),
            pltpu.SMEM((n_tiles, 2), jnp.int32),
            pltpu.SMEM((1, 1), jnp.int32),
            pltpu.SMEM((n_inner, 2), jnp.int32),
            pltpu.SMEM((n_tiles + 2 * n_inner, part_rows // tile), f32),
            pltpu.VMEM((n_inner, tile, tile), f32),
            pltpu.VMEM((2, n_face), jnp.int32),
            pltpu.VMEM((2, n_face), jnp.int32),
            pltpu.VMEM((2, n_face), jnp.int32),
            pltpu.VMEM((n_face, n_face), f32),
            pltpu.VMEM((n_face, n_face), f32),
            pltpu.VMEM((n_tiles, tile, tile), f32),
            pltpu.VMEM((n_tiles, tile, 2 * width), bf16),
            pltpu.VMEM((n_tiles, 2 * tile, width), bf16),
            pltpu.VMEM((n_tiles + 2 * n_inner, tile, width), f32),
            pltpu.VMEM((2 * n_inner, tile, tile), bf16),
            pltpu.VMEM((2 * n_inner, tile, tile), bf16),
            pltpu.VMEM((2, part_rows, part_rows), bf16),
            pltpu.VMEM((2, part_rows, part_rows), bf16),
            pltpu.VMEM((part_rows, width), f32),
            pltpu.VMEM((part_rows, width), f32),
            pltpu.VMEM((part_rows // tile, tile, 2 * width), bf16),
            pltpu.VMEM((2, 3, 1, width), f32),
            pltpu.VMEM((2, window, 1, width), f32),
            pltpu.VMEM((2, 2, 1, width), f32),
            pltpu.VMEM((2, n_bin - 1, 1, width), f32),
            dma((10,)),
            dma((APPLIES,)),
            dma((APPLIES, n_bin)),
            dma((APPLIES,)),
            dma((APPLIES,)),
            dma((APPLIES,)),
            dma((APPLIES,)),
            dma((APPLIES,)),
            dma((APPLIES,)),
            dma((3,)),
            dma((3,)),
            dma((2, 3)),
            dma((2, 3)),
        ],
        compiler_params=pltpu.CompilerParams(collective_id=0, has_side_effects=True),
    )
    return call(
        start_factors,
        bin_factors.reshape(-1, tile, width),
        tile_speed[0, 0],
        tile_weight[0, 0],
        tile_cells[0, 0],
        tile_count,
        inner_pairs[0, 0],
        inner_weight[0, 0],
        listed,
        face_weight[0, 0],
    )


def solution(mesh):
    lead = ("groups", "seg")
    rows = P(("groups", "seg", "bin"), None)
    in_specs = (
        rows,
        P(("groups", "bin"), None),
        P(lead, "bin", None, None, None),
        P(lead, "bin", None, None, None),
        P(lead, "bin", None, None),
        P(lead, "bin"),
        P(lead, "bin", None, None),
        P(lead, "bin", None, None, None),
        P(lead, "bin", None, None),
        P(lead, "bin", None),
        P(lead, "bin", None, None),
    )
    body = functools.partial(shards, mesh.shape["bin"], mesh.shape["seg"])
    return jax.shard_map(
        body, mesh=mesh, in_specs=in_specs, out_specs=(rows, rows), check_vma=False
    )
```

```python
import functools

import jax
import jax.numpy as jnp
from jax import lax
from jax.experimental import pallas as pl
from jax.experimental.pallas import tpu as pltpu
from jax.sharding import PartitionSpec as P

RIDGE = 0.5
APPLIES = 3
MESH = pl.DeviceIdType.MESH
f32 = jnp.float32
bf16 = jnp.bfloat16


def split(x):
    hi = x.astype(bf16)
    return hi, (x - hi.astype(f32)).astype(bf16)


def dot_nn(a, b):
    return jnp.dot(a, b, preferred_element_type=f32)


def dot_nt(a, b):
    return lax.dot_general(a, b, (((1,), (1,)), ((), ())), preferred_element_type=f32)


def kernel(
    n_bin,
    n_seg,
    x0_hbm,
    bins_hbm,
    speed_hbm,
    weight_hbm,
    cells_hbm,
    count_hbm,
    pairs_hbm,
    inner_hbm,
    rows_hbm,
    lives_hbm,
    face_hbm,
    step_ref,
    later_ref,
    along_ref,
    field,
    below,
    above,
    part,
    landed,
    halves,
    fulls,
    passed,
    bins,
    speed,
    weight,
    cells,
    count,
    pairs,
    hits,
    inner,
    lives,
    listed,
    rows,
    rows_below,
    rows_above,
    face,
    face_above,
    gain,
    v_wide,
    v_tall,
    pulled,
    w_hi,
    w_lo,
    f_below,
    f_above,
    degree,
    rhs,
    wide,
    sums_mine,
    sums_seg,
    sums_far,
    sums_bin,
    load_sem,
    gather_send,
    gather_recv,
    below_send,
    below_recv,
    above_send,
    above_recv,
    scatter_send,
    scatter_recv,
    setup_send,
    setup_recv,
    sums_send,
    sums_recv,
):
    seg = lax.axis_index("seg")
    bin_ = lax.axis_index("bin")
    own = x0_hbm.shape[0]
    width = x0_hbm.shape[1]
    n_tiles = speed.shape[0]
    tile = speed.shape[1]
    n_inner = inner.shape[0]
    part_rows = own * n_bin
    n_blocks = part_rows // tile
    half = n_seg // 4
    seg_next = lax.rem(seg + 1, n_seg)
    seg_prev = lax.rem(seg + n_seg - 1, n_seg)

    def seg_at(offset):
        return lax.rem(seg + (offset + n_seg), n_seg)

    def bin_at(offset):
        return lax.rem(bin_ + offset, n_bin)

    def own_slice():
        return pl.ds(pl.multiple_of(bin_ * own, own), own)

    barrier = pltpu.get_barrier_semaphore()
    seg_offsets = [d for d in range(-half, half + 1) if d != 0]
    pairs_of = (
        (x0_hbm, field.at[0, own_slice()]),
        (rows_hbm, listed),
        (lives_hbm, lives),
        (face_hbm, face),
        (cells_hbm, cells),
        (count_hbm, count),
        (pairs_hbm, pairs),
        (bins_hbm, bins),
        (weight_hbm, weight),
        (speed_hbm, speed),
        (inner_hbm, inner),
    )
    loads = [pltpu.make_async_copy(src, dst, load_sem.at[at]) for at, (src, dst) in enumerate(pairs_of)]
    loads[0].start()
    for d in range(1, n_bin):
        pl.semaphore_signal(barrier, inc=1, device_id={"bin": bin_at(d)}, device_id_type=MESH)
    for d in seg_offsets:
        pl.semaphore_signal(barrier, inc=1, device_id={"seg": seg_at(d)}, device_id_type=MESH)
    for load in loads[1:]:
        load.start()

    def slots_and_gain():
        for load in loads[4:9]:
            load.wait()
        targets = [cells[0, k] for k in range(n_tiles)]
        targets += [pairs[j // 2, j % 2] for j in range(2 * n_inner)]
        for item, target in enumerate(targets):
            for b in range(n_blocks):
                away = target - b
                hits[item, b] = (1 - jnp.minimum(away * away, 1)).astype(f32)
        for k in range(n_tiles):
            live = jnp.clip(count[0, 0] - k, 0, 1).astype(f32)
            gain[k] = weight[k].astype(f32) * live
            chosen = bins[cells[1, k]]
            v_wide[k, :, :width] = chosen
            v_wide[k, :, width:] = chosen
            v_tall[k, :tile] = chosen
            v_tall[k, tile:] = chosen

    def add_up(items, block):
        total = None
        for ref_at, item in items:
            term = ref_at() * hits[item, block]
            total = term if total is None else total + term
        return total

    def right_side():
        loads[9].wait()
        for k in range(n_tiles):
            weighted = (weight[k].astype(f32) * speed[k].astype(f32)).astype(bf16)
            live = jnp.clip(count[0, 0] - k, 0, 1).astype(f32)
            pulled[k] = dot_nn(weighted, v_tall[k, :tile]) * live
        for b in range(n_blocks):
            items = [((lambda k=k: pulled[k]), k) for k in range(n_tiles)]
            rhs[b * tile : (b + 1) * tile] = add_up(items, b)

    def inner_setup():
        loads[10].wait()
        for j in range(n_inner):
            forward = inner[j]
            hi, lo = split(forward)
            w_hi[2 * j] = hi
            w_lo[2 * j] = lo
            back = forward.T
            hi, lo = split(back)
            w_hi[2 * j + 1] = hi
            w_lo[2 * j + 1] = lo
            pulled[2 * j] = jnp.broadcast_to(forward.sum(1, keepdims=True), (tile, width))
            pulled[2 * j + 1] = jnp.broadcast_to(back.sum(1, keepdims=True), (tile, width))

    def inner_degree(b):
        items = [((lambda j=j: pulled[j]), n_tiles + j) for j in range(2 * n_inner)]
        return add_up(items, b)

    def one_hot(row_ref, which):
        n_face = row_ref.shape[1]
        listed = jnp.broadcast_to(row_ref[which : which + 1, :], (part_rows, n_face))
        at = lax.broadcasted_iota(jnp.int32, (part_rows, n_face), 0)
        return jnp.where(listed == at, 1.0, 0.0).astype(bf16)

    def face_setup():
        low_own = one_hot(rows, 0)
        up_own = one_hot(rows, 1)
        up_below = one_hot(rows_below, 1)
        low_above = one_hot(rows_above, 0)
        down = jnp.where(seg > 0, 1.0, 0.0).astype(f32)
        up = jnp.where(seg < n_seg - 1, 1.0, 0.0).astype(f32)
        mine = split(face[...] * down)
        theirs = split(face_above[...] * up)
        degrees = jnp.zeros((part_rows, 1), f32)
        for p in range(2):
            picked = dot_nn(low_own, mine[p]).astype(bf16)
            whole = dot_nt(picked, up_below)
            f_below[p] = whole.astype(bf16)
            degrees = degrees + whole.sum(1, keepdims=True)
            picked = dot_nt(up_own, theirs[p]).astype(bf16)
            whole = dot_nt(picked, low_above)
            f_above[p] = whole.astype(bf16)
            degrees = degrees + whole.sum(1, keepdims=True)
        degree[...] = jnp.broadcast_to(degrees, (part_rows, width))
        for b in range(n_blocks):
            degree[b * tile : (b + 1) * tile] += inner_degree(b)

    def doubled(product):
        return product[:, :width] + product[:, width:]

    def local_terms(step):
        hi, lo = split(field[step])
        for b in range(n_blocks):
            wide[b, :, :width] = hi[b * tile : (b + 1) * tile]
            wide[b, :, width:] = lo[b * tile : (b + 1) * tile]
        for k in range(n_tiles):
            picked = wide[cells[0, k]]
            scores = dot_nt(picked, v_wide[k]) * gain[k]
            hi, lo = split(scores)
            pulled[k] = dot_nn(jnp.concatenate([hi, lo], axis=1), v_tall[k])
        for j in range(n_inner):
            for way in range(2):
                picked = wide[pairs[j, 1 - way]]
                product = doubled(dot_nn(w_hi[2 * j + way], picked))
                product = product + dot_nn(w_lo[2 * j + way], picked[:, :width])
                pulled[n_tiles + 2 * j + way] = -product

    def face_terms(step):
        total = None
        for matrix, source in ((f_below, below), (f_above, above)):
            hi, lo = split(source[step])
            both = jnp.concatenate([hi, lo], axis=1)
            product = doubled(dot_nn(matrix[0], both)) + dot_nn(matrix[1], hi)
            total = product if total is None else total + product
        return total

    def join(step, faces):
        items = [((lambda k=k: pulled[k]), k) for k in range(n_tiles)]
        for j in range(2 * n_inner):
            items.append(((lambda j=j: pulled[n_tiles + j]), n_tiles + j))
        for b in range(n_blocks):
            at = slice(b * tile, (b + 1) * tile)
            value = add_up(items, b) + degree[at] * field[step, at] - faces[at]
            part[step, at] = rhs[at] - value if step == 0 else value

    order = sorted(range(1, n_bin), key=lambda d: -min(d, n_bin - d))

    def to_bin(src, dst, send, recv, d):
        return pltpu.make_async_remote_copy(
            src_ref=src, dst_ref=dst, send_sem=send, recv_sem=recv,
            device_id={"bin": bin_at(d)}, device_id_type=MESH,
        )

    def to_seg(src, dst, send, recv, where):
        return pltpu.make_async_remote_copy(
            src_ref=src, dst_ref=dst, send_sem=send, recv_sem=recv,
            device_id={"seg": where}, device_id_type=MESH,
        )

    def forward(step, source):
        rows_at = pl.ds(pl.multiple_of(source * own, own), own)
        block = field.at[step, rows_at]
        to_seg(block, below.at[step, rows_at], below_send.at[step], below_recv.at[step], seg_next).start()
        to_seg(block, above.at[step, rows_at], above_send.at[step], above_recv.at[step], seg_prev).start()

    slot_of = {-1: 0, 1: 1, -2: 2, 2: 3, -3: 4, 3: 5, -4: 6, 4: 7}

    def block_rows(offset, part_of=None):
        at = lax.rem(bin_ + (offset + n_bin), n_bin) * own
        size = own if part_of is None else own // 2
        if part_of:
            at = at + size
        return pl.ds(pl.multiple_of(at, size), size)

    def gather_send_to(step, source, to, part_of=None):
        block = field.at[step, block_rows(source, part_of)]
        recv = gather_recv.at[step, slot_of[source - to]]
        to_bin(block, block, gather_send.at[step], recv, to + n_bin).start()

    def gather_wait(step, source, part_of=None):
        block = field.at[step, block_rows(source, part_of)]
        pltpu.make_async_copy(block, block, gather_recv.at[step, slot_of[source]]).wait()
        rows_at = block_rows(source, part_of)
        to_seg(block, below.at[step, rows_at], below_send.at[step], below_recv.at[step], seg_next).start()
        to_seg(block, above.at[step, rows_at], above_send.at[step], above_recv.at[step], seg_prev).start()

    def gather_start(step):
        for to in (2, -2, 1, -1):
            gather_send_to(step, 0, to)
        forward(step, bin_)

    def gather_relay(step):
        for side in (-1, 1):
            source = 2 * side
            block = field.at[step, block_rows(source)]
            pltpu.make_async_copy(block, block, gather_recv.at[step, slot_of[source]]).wait()
            gather_send_to(step, source, -side)
            gather_send_to(step, source, -2 * side, 0 if side < 0 else 1)
            forward(step, lax.rem(bin_ + (source + n_bin), n_bin))
        gather_wait(step, -1)
        gather_wait(step, 1)

    def gather_finish(step):
        gather_wait(step, -3)
        gather_wait(step, 3)
        gather_wait(step, -4, 0)
        gather_wait(step, 4, 1)

    def faces_finish(step):
        pltpu.make_async_copy(below.at[step], below.at[step], below_recv.at[step]).wait()
        pltpu.make_async_copy(above.at[step], above.at[step], above_recv.at[step]).wait()

    def scatter_send_to(step, src, dst, slot, to):
        to_bin(src, dst, scatter_send.at[step], scatter_recv.at[step, slot], to + n_bin).start()

    def scatter_start(step):
        for side in (-1, 1):
            at = 0 if side < 0 else 1
            scatter_send_to(step, part.at[step, block_rows(4, 1 - at)], halves.at[step, at], at, 2 * side)
            scatter_send_to(step, part.at[step, block_rows(3 * side)], fulls.at[step, at], 2 + at, side)
        for side in (-1, 1):
            at = 0 if side < 0 else 1
            scatter_send_to(step, part.at[step, block_rows(side)], landed.at[step, at], 4 + at, side)

    def arrived(step, ref, slot):
        pltpu.make_async_copy(ref, ref, scatter_recv.at[step, slot]).wait()

    def scatter_relay(step):
        for side in (-1, 1):
            at = 0 if side < 0 else 1
            size = own // 2
            arrived(step, fulls.at[step, at], 2 + at)
            arrived(step, halves.at[step, at], at)
            total = part[step, block_rows(2 * side)] + fulls[step, at]
            other = 1 - at
            mine = slice(other * size, (other + 1) * size)
            rest = slice(at * size, (at + 1) * size)
            passed[step, at, rest] = total[rest]
            passed[step, at, mine] = total[mine] + halves[step, at]
            scatter_send_to(step, passed.at[step, at], landed.at[step, 2 + at], 6 + at, 2 * side)

    def scatter_finish(step):
        total = part[step, own_slice()]
        for at in range(4):
            arrived(step, landed.at[step, at], 4 + at)
            total = total + landed[step, at]
        return total

    window = [e for e in range(-half + 1, half + 1) if e != 0]

    def two_sums(first, second):
        lanes = lax.broadcasted_iota(jnp.int32, (1, width), 1)
        first = first.sum(0, keepdims=True)
        second = second.sum(0, keepdims=True)
        first = first + pltpu.roll(first, width // 2, 1)
        second = second + pltpu.roll(second, width // 2, 1)
        return jnp.where(lanes < width // 2, first, second)

    def sums_start(turn, value):
        sums_mine[turn, 0] = value
        for at, e in enumerate(window):
            to_seg(sums_mine.at[turn, 0], sums_seg.at[turn, at], sums_send.at[turn, 0], sums_recv.at[turn, 0], seg_at(e)).start()

    def sums_second(turn):
        pltpu.make_async_copy(sums_seg.at[turn], sums_seg.at[turn], sums_recv.at[turn, 0]).wait()
        total = sums_mine[turn, 0]
        for at in range(len(window)):
            total = total + sums_seg[turn, at]
        sums_mine[turn, 1] = total
        for at, e in enumerate((-half, half)):
            to_seg(sums_mine.at[turn, 1], sums_far.at[turn, at], sums_send.at[turn, 1], sums_recv.at[turn, 1], seg_at(e)).start()

    def sums_third(turn):
        pltpu.make_async_copy(sums_far.at[turn], sums_far.at[turn], sums_recv.at[turn, 1]).wait()
        total = sums_far[turn, 0] + sums_far[turn, 1]
        sums_mine[turn, 2] = total
        for d in order:
            to_bin(sums_mine.at[turn, 2], sums_bin.at[turn, d - 1], sums_send.at[turn, 2], sums_recv.at[turn, 2], d).start()

    def sums_finish(turn):
        pltpu.make_async_copy(sums_bin.at[turn], sums_bin.at[turn], sums_recv.at[turn, 2]).wait()
        total = sums_mine[turn, 2]
        for d in range(n_bin - 1):
            total = total + sums_bin[turn, d]
        lanes = lax.broadcasted_iota(jnp.int32, (1, width), 1)
        first = jnp.sum(jnp.where(lanes < width // 2, total, 0.0), axis=1, keepdims=True)
        second = jnp.sum(jnp.where(lanes < width // 2, 0.0, total), axis=1, keepdims=True)
        return first, second

    for load in loads[1:3]:
        load.wait()
    slot_at = lax.broadcasted_iota(jnp.int32, (1, listed.shape[1]), 1)
    for side in range(2):
        own_list = listed[side : side + 1, :]
        rows[side : side + 1, :] = jnp.where(slot_at < lives[0, side], own_list, -1)
    loads[0].wait()
    loads[3].wait()
    pl.semaphore_wait(barrier, n_bin - 1 + len(seg_offsets))
    to_seg(face, face_above, setup_send.at[2], setup_recv.at[2], seg_prev).start()
    gather_start(0)
    to_seg(rows, rows_below, setup_send.at[0], setup_recv.at[0], seg_next).start()
    to_seg(rows, rows_above, setup_send.at[1], setup_recv.at[1], seg_prev).start()
    slots_and_gain()
    right_side()
    gather_relay(0)
    inner_setup()
    pltpu.make_async_copy(rows, rows_below, setup_recv.at[0]).wait()
    pltpu.make_async_copy(rows, rows_above, setup_recv.at[1]).wait()
    pltpu.make_async_copy(face, face_above, setup_recv.at[2]).wait()
    face_setup()
    gather_finish(0)
    local_terms(0)
    faces_finish(0)
    join(0, face_terms(0))
    scatter_start(0)
    scatter_relay(0)
    start = field[0, own_slice()]
    residual = scatter_finish(0) - RIDGE * start
    field[1, own_slice()] = residual

    gather_start(1)
    gather_relay(1)
    gather_finish(1)
    local_terms(1)
    faces_finish(1)
    join(1, face_terms(1))
    square = residual * residual
    sums_start(0, two_sums(square, field[1] * part[1]))
    scatter_start(1)
    scatter_relay(1)
    sums_second(0)
    image = scatter_finish(1) + RIDGE * field[1, own_slice()]
    field[2, own_slice()] = image
    gather_start(2)
    gather_relay(2)
    sums_third(0)

    gather_finish(2)
    local_terms(2)
    faces_finish(2)
    join(2, face_terms(2))
    norm, product = sums_finish(0)
    product = product + RIDGE * norm
    step_one = norm / product
    residual = field[1, own_slice()]
    image = field[2, own_slice()]
    later = residual - step_one * image
    whole = field[1] - step_one * field[2]
    whole_image = part[1] - step_one * part[2]
    sums_start(1, two_sums(later * later, whole * whole_image))
    scatter_start(2)
    scatter_relay(2)
    sums_second(1)
    sums_third(1)
    image_two = scatter_finish(2) + RIDGE * field[2, own_slice()]
    norm_next, product_next = sums_finish(1)
    product_next = product_next + RIDGE * norm_next
    beta = norm_next / norm
    step_two = norm_next / (product_next - beta * norm_next / step_one)
    residual = field[1, own_slice()]
    image = field[2, own_slice()]
    later = residual - step_one * image
    later_image = image - step_one * image_two
    direction = later + beta * residual
    along = later_image + beta * image
    step_ref[...] = step_one * residual + step_two * direction
    later_ref[...] = later
    along_ref[...] = step_two * along

    pltpu.make_async_copy(rows, rows, setup_send.at[0]).wait()
    pltpu.make_async_copy(rows, rows, setup_send.at[1]).wait()
    pltpu.make_async_copy(face, face, setup_send.at[2]).wait()
    for step in range(APPLIES):
        sent = field.at[step, : (n_bin - 1) * own]
        pltpu.make_async_copy(sent, sent, gather_send.at[step]).wait()
        pltpu.make_async_copy(sent, sent, scatter_send.at[step]).wait()
        pltpu.make_async_copy(below.at[step], below.at[step], below_send.at[step]).wait()
        pltpu.make_async_copy(above.at[step], above.at[step], above_send.at[step]).wait()
    for turn in range(2):
        pltpu.make_async_copy(sums_seg.at[turn], sums_seg.at[turn], sums_send.at[turn, 0]).wait()
        pltpu.make_async_copy(sums_far.at[turn], sums_far.at[turn], sums_send.at[turn, 1]).wait()
        pltpu.make_async_copy(sums_bin.at[turn], sums_bin.at[turn], sums_send.at[turn, 2]).wait()


def shards(
    n_bin,
    n_seg,
    start_factors,
    bin_factors,
    tile_speed,
    tile_weight,
    tile_cells,
    tile_count,
    inner_pairs,
    inner_weight,
    face_rows,
    face_count,
    face_weight,
):
    own, width = start_factors.shape
    n_tiles, tile = tile_speed.shape[2:4]
    n_inner = inner_weight.shape[2]
    n_face = face_rows.shape[3]
    part_rows = own * n_bin
    half = n_seg // 4
    window = 2 * half - 1
    any_ = pl.BlockSpec(memory_space=pl.ANY)
    vmem = pl.BlockSpec(memory_space=pltpu.VMEM)
    dma = pltpu.SemaphoreType.DMA
    out = jax.ShapeDtypeStruct((own, width), f32)
    call = pl.pallas_call(
        functools.partial(kernel, n_bin, n_seg),
        out_shape=(out, out, out),
        in_specs=[any_] * 11,
        out_specs=(vmem, vmem, vmem),
        scratch_shapes=[
            pltpu.VMEM((APPLIES, part_rows, width), f32),
            pltpu.VMEM((APPLIES, part_rows, width), f32),
            pltpu.VMEM((APPLIES, part_rows, width), f32),
            pltpu.VMEM((APPLIES, part_rows, width), f32),
            pltpu.VMEM((APPLIES, 4, own, width), f32),
            pltpu.VMEM((APPLIES, 2, own // 2, width), f32),
            pltpu.VMEM((APPLIES, 2, own, width), f32),
            pltpu.VMEM((APPLIES, 2, own, width), f32),
            pltpu.VMEM((bin_factors.shape[0] // tile, tile, width), bf16),
            pltpu.VMEM((n_tiles, tile, tile), bf16),
            pltpu.VMEM((n_tiles, tile, tile), bf16),
            pltpu.SMEM((2, n_tiles), jnp.int32),
            pltpu.SMEM((1, 1), jnp.int32),
            pltpu.SMEM((n_inner, 2), jnp.int32),
            pltpu.SMEM((n_tiles + 2 * n_inner, part_rows // tile), f32),
            pltpu.VMEM((n_inner, tile, tile), f32),
            pltpu.SMEM((1, 2), jnp.int32),
            pltpu.VMEM((2, n_face), jnp.int32),
            pltpu.VMEM((2, n_face), jnp.int32),
            pltpu.VMEM((2, n_face), jnp.int32),
            pltpu.VMEM((2, n_face), jnp.int32),
            pltpu.VMEM((n_face, n_face), f32),
            pltpu.VMEM((n_face, n_face), f32),
            pltpu.VMEM((n_tiles, tile, tile), f32),
            pltpu.VMEM((n_tiles, tile, 2 * width), bf16),
            pltpu.VMEM((n_tiles, 2 * tile, width), bf16),
            pltpu.VMEM((n_tiles + 2 * n_inner, tile, width), f32),
            pltpu.VMEM((2 * n_inner, tile, tile), bf16),
            pltpu.VMEM((2 * n_inner, tile, tile), bf16),
            pltpu.VMEM((2, part_rows, part_rows), bf16),
            pltpu.VMEM((2, part_rows, part_rows), bf16),
            pltpu.VMEM((part_rows, width), f32),
            pltpu.VMEM((part_rows, width), f32),
            pltpu.VMEM((part_rows // tile, tile, 2 * width), bf16),
            pltpu.VMEM((2, 3, 1, width), f32),
            pltpu.VMEM((2, window, 1, width), f32),
            pltpu.VMEM((2, 2, 1, width), f32),
            pltpu.VMEM((2, n_bin - 1, 1, width), f32),
            dma((11,)),
            dma((APPLIES,)),
            dma((APPLIES, n_bin)),
            dma((APPLIES,)),
            dma((APPLIES,)),
            dma((APPLIES,)),
            dma((APPLIES,)),
            dma((APPLIES,)),
            dma((APPLIES, n_bin)),
            dma((3,)),
            dma((3,)),
            dma((2, 3)),
            dma((2, 3)),
        ],
        compiler_params=pltpu.CompilerParams(collective_id=0, has_side_effects=True),
    )
    step, later, along = call(
        start_factors,
        bin_factors.reshape(-1, tile, width),
        tile_speed[0, 0],
        tile_weight[0, 0],
        tile_cells[0, 0].T,
        tile_count,
        inner_pairs[0, 0],
        inner_weight[0, 0],
        face_rows[0, 0],
        face_count[0],
        face_weight[0, 0],
    )
    return start_factors + step, later - along


def solution(mesh):
    lead = ("groups", "seg")
    rows = P(("groups", "seg", "bin"), None)
    in_specs = (
        rows,
        P(("groups", "bin"), None),
        P(lead, "bin", None, None, None),
        P(lead, "bin", None, None, None),
        P(lead, "bin", None, None),
        P(lead, "bin"),
        P(lead, "bin", None, None),
        P(lead, "bin", None, None, None),
        P(lead, "bin", None, None),
        P(lead, "bin", None),
        P(lead, "bin", None, None),
    )
    body = functools.partial(shards, mesh.shape["bin"], mesh.shape["seg"])
    return jax.shard_map(
        body, mesh=mesh, in_specs=in_specs, out_specs=(rows, rows), check_vma=False
    )
```

```python
import functools

import jax
import jax.numpy as jnp
from jax import lax
from jax.experimental import pallas as pl
from jax.experimental.pallas import tpu as pltpu
from jax.sharding import PartitionSpec as P

RIDGE = 0.5
APPLIES = 3
MESH = pl.DeviceIdType.MESH
f32 = jnp.float32
bf16 = jnp.bfloat16


def split(x):
    hi = x.astype(bf16)
    return hi, (x - hi.astype(f32)).astype(bf16)


def dot_nn(a, b):
    return jnp.dot(a, b, preferred_element_type=f32)


def dot_nt(a, b):
    return lax.dot_general(a, b, (((1,), (1,)), ((), ())), preferred_element_type=f32)


def kernel(
    n_bin,
    n_seg,
    x0_hbm,
    bins_hbm,
    speed_hbm,
    weight_hbm,
    cells_hbm,
    count_hbm,
    pairs_hbm,
    inner_hbm,
    rows_hbm,
    lives_hbm,
    face_hbm,
    sol_ref,
    res_ref,
    field,
    below,
    above,
    part,
    landed,
    halves,
    fulls,
    passed,
    summed,
    bins,
    speed,
    weight,
    cells,
    count,
    pairs,
    hits,
    inner,
    lives,
    listed,
    rows,
    rows_below,
    rows_above,
    face,
    face_above,
    gain,
    v_wide,
    v_tall,
    pulled,
    w_hi,
    w_lo,
    f_below,
    f_above,
    degree,
    rhs,
    base,
    wide,
    sums_mine,
    sums_seg,
    sums_far,
    sums_all,
    sums_bin,
    load_sem,
    gather_send,
    gather_recv,
    below_send,
    below_recv,
    above_send,
    above_recv,
    scatter_send,
    scatter_recv,
    setup_send,
    setup_recv,
    sums_send,
    sums_recv,
):
    seg = lax.axis_index("seg")
    bin_ = lax.axis_index("bin")
    own = x0_hbm.shape[0]
    width = x0_hbm.shape[1]
    n_tiles = speed.shape[0]
    tile = speed.shape[1]
    n_inner = inner.shape[0]
    part_rows = own * n_bin
    n_blocks = part_rows // tile
    half = n_seg // 4
    seg_next = lax.rem(seg + 1, n_seg)
    seg_prev = lax.rem(seg + n_seg - 1, n_seg)

    def seg_at(offset):
        return lax.rem(seg + (offset + n_seg), n_seg)

    def bin_at(offset):
        return lax.rem(bin_ + offset, n_bin)

    def own_slice():
        return pl.ds(pl.multiple_of(bin_ * own, own), own)

    barrier = pltpu.get_barrier_semaphore()
    seg_offsets = [d for d in range(-half, half + 1) if d != 0]
    pairs_of = (
        (x0_hbm, field.at[0, own_slice()]),
        (rows_hbm, listed),
        (lives_hbm, lives),
        (face_hbm, face),
        (cells_hbm, cells),
        (count_hbm, count),
        (pairs_hbm, pairs),
        (bins_hbm, bins),
        (weight_hbm, weight),
        (speed_hbm, speed),
        (inner_hbm, inner),
    )
    loads = [pltpu.make_async_copy(src, dst, load_sem.at[at]) for at, (src, dst) in enumerate(pairs_of)]
    loads[0].start()
    for d in range(1, n_bin):
        pl.semaphore_signal(barrier, inc=1, device_id={"bin": bin_at(d)}, device_id_type=MESH)
    for d in seg_offsets:
        pl.semaphore_signal(barrier, inc=1, device_id={"seg": seg_at(d)}, device_id_type=MESH)
    for load in loads[1:]:
        load.start()

    def slots_and_gain():
        for load in loads[4:9]:
            load.wait()
        targets = [cells[0, k] for k in range(n_tiles)]
        targets += [pairs[j // 2, j % 2] for j in range(2 * n_inner)]
        for item, target in enumerate(targets):
            for b in range(n_blocks):
                away = target - b
                hits[item, b] = (1 - jnp.minimum(away * away, 1)).astype(f32)
        for k in range(n_tiles):
            live = jnp.clip(count[0, 0] - k, 0, 1).astype(f32)
            gain[k] = weight[k].astype(f32) * live
            chosen = bins[cells[1, k]]
            v_wide[k, :, :width] = chosen
            v_wide[k, :, width:] = chosen
            v_tall[k, :tile] = chosen
            v_tall[k, tile:] = chosen

    def add_up(items, block):
        total = None
        for ref_at, item in items:
            term = ref_at() * hits[item, block]
            total = term if total is None else total + term
        return total

    def right_side():
        loads[9].wait()
        for k in range(n_tiles):
            weighted = (weight[k].astype(f32) * speed[k].astype(f32)).astype(bf16)
            live = jnp.clip(count[0, 0] - k, 0, 1).astype(f32)
            pulled[k] = dot_nn(weighted, v_tall[k, :tile]) * live
        for b in range(n_blocks):
            items = [((lambda k=k: pulled[k]), k) for k in range(n_tiles)]
            rhs[b * tile : (b + 1) * tile] = add_up(items, b)

    def inner_setup():
        loads[10].wait()
        for j in range(n_inner):
            forward = inner[j]
            hi, lo = split(forward)
            w_hi[2 * j] = hi
            w_lo[2 * j] = lo
            back = forward.T
            hi, lo = split(back)
            w_hi[2 * j + 1] = hi
            w_lo[2 * j + 1] = lo
            pulled[2 * j] = jnp.broadcast_to(forward.sum(1, keepdims=True), (tile, width))
            pulled[2 * j + 1] = jnp.broadcast_to(back.sum(1, keepdims=True), (tile, width))

    def inner_degree(b):
        items = [((lambda j=j: pulled[j]), n_tiles + j) for j in range(2 * n_inner)]
        return add_up(items, b)

    def one_hot(row_ref, which):
        n_face = row_ref.shape[1]
        listed = jnp.broadcast_to(row_ref[which : which + 1, :], (part_rows, n_face))
        at = lax.broadcasted_iota(jnp.int32, (part_rows, n_face), 0)
        return jnp.where(listed == at, 1.0, 0.0).astype(bf16)

    def face_setup():
        low_own = one_hot(rows, 0)
        up_own = one_hot(rows, 1)
        up_below = one_hot(rows_below, 1)
        low_above = one_hot(rows_above, 0)
        down = jnp.where(seg > 0, 1.0, 0.0).astype(f32)
        up = jnp.where(seg < n_seg - 1, 1.0, 0.0).astype(f32)
        mine = split(face[...] * down)
        theirs = split(face_above[...] * up)
        degrees = jnp.zeros((part_rows, 1), f32)
        for p in range(2):
            picked = dot_nn(low_own, mine[p]).astype(bf16)
            whole = dot_nt(picked, up_below)
            f_below[p] = whole.astype(bf16)
            degrees = degrees + whole.sum(1, keepdims=True)
            picked = dot_nt(up_own, theirs[p]).astype(bf16)
            whole = dot_nt(picked, low_above)
            f_above[p] = whole.astype(bf16)
            degrees = degrees + whole.sum(1, keepdims=True)
        degree[...] = jnp.broadcast_to(degrees, (part_rows, width))
        for b in range(n_blocks):
            degree[b * tile : (b + 1) * tile] += inner_degree(b)

    def doubled(product):
        return product[:, :width] + product[:, width:]

    def local_terms(step):
        hi, lo = split(field[step])
        for b in range(n_blocks):
            wide[b, :, :width] = hi[b * tile : (b + 1) * tile]
            wide[b, :, width:] = lo[b * tile : (b + 1) * tile]
        for k in range(n_tiles):
            picked = wide[cells[0, k]]
            scores = dot_nt(picked, v_wide[k]) * gain[k]
            hi, lo = split(scores)
            pulled[k] = dot_nn(jnp.concatenate([hi, lo], axis=1), v_tall[k])
        for j in range(n_inner):
            for way in range(2):
                picked = wide[pairs[j, 1 - way]]
                product = doubled(dot_nn(w_hi[2 * j + way], picked))
                product = product + dot_nn(w_lo[2 * j + way], picked[:, :width])
                pulled[n_tiles + 2 * j + way] = -product

    def face_term(step, matrix, source):
        hi, lo = split(source[step])
        both = jnp.concatenate([hi, lo], axis=1)
        return doubled(dot_nn(matrix[0], both)) + dot_nn(matrix[1], hi)

    def base_terms(step):
        items = [((lambda k=k: pulled[k]), k) for k in range(n_tiles)]
        for j in range(2 * n_inner):
            items.append(((lambda j=j: pulled[n_tiles + j]), n_tiles + j))
        for b in range(n_blocks):
            at = slice(b * tile, (b + 1) * tile)
            value = add_up(items, b) + degree[at] * field[step, at]
            base[at] = value

    def join(step, faces):
        value = base[...] - faces
        part[step] = rhs[...] - value if step == 0 else value

    order = sorted(range(1, n_bin), key=lambda d: -min(d, n_bin - d))

    def to_bin(src, dst, send, recv, d):
        return pltpu.make_async_remote_copy(
            src_ref=src, dst_ref=dst, send_sem=send, recv_sem=recv,
            device_id={"bin": bin_at(d)}, device_id_type=MESH,
        )

    def to_seg(src, dst, send, recv, where):
        return pltpu.make_async_remote_copy(
            src_ref=src, dst_ref=dst, send_sem=send, recv_sem=recv,
            device_id={"seg": where}, device_id_type=MESH,
        )

    direct = lax.rem(seg, 2) == 0
    tree = jnp.logical_not(direct)
    slot_of = {-1: 0, 1: 1, -2: 2, 2: 3, -3: 4, 3: 5, -4: 6, 4: 7}
    straight = (4, 3, -3, 2, -2, 1, -1)

    def block_rows(offset, part_of=None):
        at = lax.rem(bin_ + (offset + n_bin), n_bin) * own
        size = own if part_of is None else own // 2
        if part_of:
            at = at + size
        return pl.ds(pl.multiple_of(at, size), size)

    def gather_send_to(step, source, to, part_of=None):
        block = field.at[step, block_rows(source, part_of)]
        recv = gather_recv.at[step, slot_of[source - to]]
        to_bin(block, block, gather_send.at[step], recv, to + n_bin).start()

    def gather_take(step, source, part_of=None):
        block = field.at[step, block_rows(source, part_of)]
        pltpu.make_async_copy(block, block, gather_recv.at[step, slot_of[source]]).wait()

    def pass_on(step, source, part_of=None):
        rows_at = block_rows(source, part_of)
        block = field.at[step, rows_at]
        to_seg(block, below.at[step, rows_at], below_send.at[step], below_recv.at[step], seg_next).start()
        to_seg(block, above.at[step, rows_at], above_send.at[step], above_recv.at[step], seg_prev).start()

    def gather_start(step):
        @pl.when(direct)
        def _():
            for to in straight:
                gather_send_to(step, 0, to)

        @pl.when(tree)
        def _():
            for to in (2, -2, 1, -1):
                gather_send_to(step, 0, to)

        pass_on(step, 0)

    def gather_relay(step):
        @pl.when(direct)
        def _():
            for source in (3, 2, -3, -2):
                gather_take(step, source)
                pass_on(step, source)

        @pl.when(tree)
        def _():
            for side in (-1, 1):
                source = 2 * side
                gather_take(step, source)
                gather_send_to(step, source, -side)
                gather_send_to(step, source, -2 * side, 0 if side < 0 else 1)
                pass_on(step, source)
            for source in (-1, 1):
                gather_take(step, source)
                pass_on(step, source)

    def gather_finish(step):
        @pl.when(direct)
        def _():
            for source in (1, -1, -4):
                gather_take(step, source)
                pass_on(step, source)

        @pl.when(tree)
        def _():
            for source, part_of in ((-3, None), (3, None), (-4, 0), (4, 1)):
                gather_take(step, source, part_of)
                pass_on(step, source, part_of)

    def faces_join(step):
        def one(matrix, source, recv):
            pltpu.make_async_copy(source.at[step], source.at[step], recv.at[step]).wait()
            return face_term(step, matrix, source)

        @pl.when(direct)
        def _():
            base[...] -= one(f_above, above, above_recv)
            join(step, one(f_below, below, below_recv))

        @pl.when(tree)
        def _():
            base[...] -= one(f_below, below, below_recv)
            join(step, one(f_above, above, above_recv))

    def scatter_send_to(step, src, dst, slot, to):
        to_bin(src, dst, scatter_send.at[step], scatter_recv.at[step, slot], to + n_bin).start()

    def scatter_start(step):
        @pl.when(direct)
        def _():
            for slot, to in enumerate(straight):
                block = part.at[step, block_rows(to)]
                scatter_send_to(step, block, landed.at[step, slot], slot, to)

        @pl.when(tree)
        def _():
            for at, side in enumerate((-1, 1)):
                far = part.at[step, block_rows(4, 1 - at)]
                scatter_send_to(step, far, halves.at[step, at], 4 + at, 2 * side)
                near = part.at[step, block_rows(3 * side)]
                scatter_send_to(step, near, fulls.at[step, at], 6 + at, side)
            for at, side in enumerate((-1, 1)):
                block = part.at[step, block_rows(side)]
                scatter_send_to(step, block, landed.at[step, at], at, side)

    def arrived(step, ref, slot):
        pltpu.make_async_copy(ref, ref, scatter_recv.at[step, slot]).wait()

    def scatter_relay(step):
        @pl.when(tree)
        def _():
            size = own // 2
            for at, side in enumerate((-1, 1)):
                arrived(step, fulls.at[step, at], 6 + at)
                arrived(step, halves.at[step, at], 4 + at)
                total = part[step, block_rows(2 * side)] + fulls[step, at]
                mine = slice((1 - at) * size, (2 - at) * size)
                rest = slice(at * size, (at + 1) * size)
                passed[step, at, rest] = total[rest]
                passed[step, at, mine] = total[mine] + halves[step, at]
                scatter_send_to(step, passed.at[step, at], landed.at[step, 2 + at], 2 + at, 2 * side)

    def scatter_finish(step):
        def add(slots):
            total = part[step, own_slice()]
            for slot in slots:
                arrived(step, landed.at[step, slot], slot)
                total = total + landed[step, slot]
            summed[...] = total

        @pl.when(direct)
        def _():
            add(range(len(straight) - 1, -1, -1))

        @pl.when(tree)
        def _():
            add(range(4))

        return summed[...]

    window = [e for e in range(-half + 1, half + 1) if e != 0]

    def two_sums(first, second):
        lanes = lax.broadcasted_iota(jnp.int32, (1, width), 1)
        first = first.sum(0, keepdims=True)
        second = second.sum(0, keepdims=True)
        first = first + pltpu.roll(first, width // 2, 1)
        second = second + pltpu.roll(second, width // 2, 1)
        return jnp.where(lanes < width // 2, first, second)

    def sums_start(turn, value):
        sums_mine[turn, 0] = value
        for at, e in enumerate(window):
            to_seg(sums_mine.at[turn, 0], sums_seg.at[at], sums_send.at[turn, 0], sums_recv.at[turn, 0], seg_at(e)).start()

    def sums_second(turn):
        pltpu.make_async_copy(sums_seg, sums_seg, sums_recv.at[turn, 0]).wait()
        total = sums_mine[turn, 0]
        for at in range(len(window)):
            total = total + sums_seg[at]
        sums_mine[turn, 1] = total
        for at, e in enumerate((-half, half)):
            to_seg(sums_mine.at[turn, 1], sums_far.at[at], sums_send.at[turn, 1], sums_recv.at[turn, 1], seg_at(e)).start()

    def sums_third(turn):
        pltpu.make_async_copy(sums_far, sums_far, sums_recv.at[turn, 1]).wait()
        sums_to_bins(turn, sums_far[0] + sums_far[1])

    def sums_start_all(turn, value):
        sums_mine[turn, 0] = value
        for e in sorted(range(1, n_seg), key=lambda e: -min(e, n_seg - e)):
            to_seg(sums_mine.at[turn, 0], sums_all.at[e - 1], sums_send.at[turn, 0], sums_recv.at[turn, 0], seg_at(e)).start()

    def sums_third_all(turn):
        pltpu.make_async_copy(sums_all, sums_all, sums_recv.at[turn, 0]).wait()
        total = sums_mine[turn, 0]
        for e in range(1, n_seg):
            total = total + sums_all[e - 1]
        sums_to_bins(turn, total)

    def sums_to_bins(turn, total):
        sums_mine[turn, 2] = total
        for d in order:
            to_bin(sums_mine.at[turn, 2], sums_bin.at[turn, d - 1], sums_send.at[turn, 2], sums_recv.at[turn, 2], d).start()

    def sums_finish(turn):
        pltpu.make_async_copy(sums_bin.at[turn], sums_bin.at[turn], sums_recv.at[turn, 2]).wait()
        total = sums_mine[turn, 2]
        for d in range(n_bin - 1):
            total = total + sums_bin[turn, d]
        lanes = lax.broadcasted_iota(jnp.int32, (1, width), 1)
        first = jnp.sum(jnp.where(lanes < width // 2, total, 0.0), axis=1, keepdims=True)
        second = jnp.sum(jnp.where(lanes < width // 2, 0.0, total), axis=1, keepdims=True)
        return first, second

    for load in loads[1:3]:
        load.wait()
    slot_at = lax.broadcasted_iota(jnp.int32, (1, listed.shape[1]), 1)
    for side in range(2):
        own_list = listed[side : side + 1, :]
        rows[side : side + 1, :] = jnp.where(slot_at < lives[0, side], own_list, -1)
    loads[0].wait()
    pl.semaphore_wait(barrier, n_bin - 1 + len(seg_offsets))
    gather_start(0)
    loads[3].wait()
    to_seg(face, face_above, setup_send.at[2], setup_recv.at[2], seg_prev).start()
    to_seg(rows, rows_below, setup_send.at[0], setup_recv.at[0], seg_next).start()
    to_seg(rows, rows_above, setup_send.at[1], setup_recv.at[1], seg_prev).start()
    slots_and_gain()
    right_side()
    gather_relay(0)
    inner_setup()
    pltpu.make_async_copy(rows, rows_below, setup_recv.at[0]).wait()
    pltpu.make_async_copy(rows, rows_above, setup_recv.at[1]).wait()
    pltpu.make_async_copy(face, face_above, setup_recv.at[2]).wait()
    face_setup()
    gather_finish(0)
    local_terms(0)
    base_terms(0)
    faces_join(0)
    scatter_start(0)
    scatter_relay(0)
    start = field[0, own_slice()]
    residual = scatter_finish(0) - RIDGE * start
    field[1, own_slice()] = residual

    gather_start(1)
    gather_relay(1)
    gather_finish(1)
    local_terms(1)
    base_terms(1)
    faces_join(1)
    square = residual * residual
    scatter_start(1)
    sums_start(0, two_sums(square, field[1] * part[1]))
    scatter_relay(1)
    sums_second(0)
    image = scatter_finish(1) + RIDGE * field[1, own_slice()]
    field[2, own_slice()] = image
    gather_start(2)
    gather_relay(2)
    sums_third(0)

    gather_finish(2)
    local_terms(2)
    base_terms(2)
    faces_join(2)
    norm, product = sums_finish(0)
    product = product + RIDGE * norm
    step_one = norm / product
    residual = field[1, own_slice()]
    image = field[2, own_slice()]
    later = residual - step_one * image
    whole = field[1] - step_one * field[2]
    whole_image = part[1] - step_one * part[2]
    sums_start_all(1, two_sums(later * later, whole * whole_image))
    scatter_start(2)
    scatter_relay(2)
    sums_third_all(1)
    image_two = scatter_finish(2) + RIDGE * field[2, own_slice()]
    norm_next, product_next = sums_finish(1)
    product_next = product_next + RIDGE * norm_next
    beta = norm_next / norm
    step_two = norm_next / (product_next - beta * norm_next / step_one)
    residual = field[1, own_slice()]
    image = field[2, own_slice()]
    later = residual - step_one * image
    later_image = image - step_one * image_two
    direction = later + beta * residual
    along = later_image + beta * image
    sol_ref[...] = field[0, own_slice()] + step_one * residual + step_two * direction
    res_ref[...] = later - step_two * along

    pltpu.make_async_copy(rows, rows, setup_send.at[0]).wait()
    pltpu.make_async_copy(rows, rows, setup_send.at[1]).wait()
    pltpu.make_async_copy(face, face, setup_send.at[2]).wait()
    for step in range(APPLIES):
        sent = field.at[step, : (n_bin - 1) * own]
        pltpu.make_async_copy(sent, sent, gather_send.at[step]).wait()
        pltpu.make_async_copy(sent, sent, scatter_send.at[step]).wait()
        pltpu.make_async_copy(below.at[step], below.at[step], below_send.at[step]).wait()
        pltpu.make_async_copy(above.at[step], above.at[step], above_send.at[step]).wait()
    pltpu.make_async_copy(sums_seg, sums_seg, sums_send.at[0, 0]).wait()
    pltpu.make_async_copy(sums_far, sums_far, sums_send.at[0, 1]).wait()
    pltpu.make_async_copy(sums_all, sums_all, sums_send.at[1, 0]).wait()
    for turn in range(2):
        pltpu.make_async_copy(sums_bin.at[turn], sums_bin.at[turn], sums_send.at[turn, 2]).wait()


def shards(
    n_bin,
    n_seg,
    start_factors,
    bin_factors,
    tile_speed,
    tile_weight,
    tile_cells,
    tile_count,
    inner_pairs,
    inner_weight,
    face_rows,
    face_count,
    face_weight,
):
    own, width = start_factors.shape
    n_tiles, tile = tile_speed.shape[2:4]
    n_inner = inner_weight.shape[2]
    n_face = face_rows.shape[3]
    part_rows = own * n_bin
    half = n_seg // 4
    window = 2 * half - 1
    any_ = pl.BlockSpec(memory_space=pl.ANY)
    vmem = pl.BlockSpec(memory_space=pltpu.VMEM)
    dma = pltpu.SemaphoreType.DMA
    call = pl.pallas_call(
        functools.partial(kernel, n_bin, n_seg),
        out_shape=(pltpu.VMEM((own, width), f32),) * 2,
        in_specs=[any_] * 11,
        out_specs=(vmem, vmem),
        scratch_shapes=[
            pltpu.VMEM((APPLIES, part_rows, width), f32),
            pltpu.VMEM((APPLIES, part_rows, width), f32),
            pltpu.VMEM((APPLIES, part_rows, width), f32),
            pltpu.VMEM((APPLIES, part_rows, width), f32),
            pltpu.VMEM((APPLIES, 7, own, width), f32),
            pltpu.VMEM((APPLIES, 2, own // 2, width), f32),
            pltpu.VMEM((APPLIES, 2, own, width), f32),
            pltpu.VMEM((APPLIES, 2, own, width), f32),
            pltpu.VMEM((own, width), f32),
            pltpu.VMEM((bin_factors.shape[0] // tile, tile, width), bf16),
            pltpu.VMEM((n_tiles, tile, tile), bf16),
            pltpu.VMEM((n_tiles, tile, tile), bf16),
            pltpu.SMEM((2, n_tiles), jnp.int32),
            pltpu.SMEM((1, 1), jnp.int32),
            pltpu.SMEM((n_inner, 2), jnp.int32),
            pltpu.SMEM((n_tiles + 2 * n_inner, part_rows // tile), f32),
            pltpu.VMEM((n_inner, tile, tile), f32),
            pltpu.SMEM((1, 2), jnp.int32),
            pltpu.VMEM((2, n_face), jnp.int32),
            pltpu.VMEM((2, n_face), jnp.int32),
            pltpu.VMEM((2, n_face), jnp.int32),
            pltpu.VMEM((2, n_face), jnp.int32),
            pltpu.VMEM((n_face, n_face), f32),
            pltpu.VMEM((n_face, n_face), f32),
            pltpu.VMEM((n_tiles, tile, tile), f32),
            pltpu.VMEM((n_tiles, tile, 2 * width), bf16),
            pltpu.VMEM((n_tiles, 2 * tile, width), bf16),
            pltpu.VMEM((n_tiles + 2 * n_inner, tile, width), f32),
            pltpu.VMEM((2 * n_inner, tile, tile), bf16),
            pltpu.VMEM((2 * n_inner, tile, tile), bf16),
            pltpu.VMEM((2, part_rows, part_rows), bf16),
            pltpu.VMEM((2, part_rows, part_rows), bf16),
            pltpu.VMEM((part_rows, width), f32),
            pltpu.VMEM((part_rows, width), f32),
            pltpu.VMEM((part_rows, width), f32),
            pltpu.VMEM((part_rows // tile, tile, 2 * width), bf16),
            pltpu.VMEM((2, 3, 1, width), f32),
            pltpu.VMEM((window, 1, width), f32),
            pltpu.VMEM((2, 1, width), f32),
            pltpu.VMEM((n_seg - 1, 1, width), f32),
            pltpu.VMEM((2, n_bin - 1, 1, width), f32),
            dma((11,)),
            dma((APPLIES,)),
            dma((APPLIES, n_bin)),
            dma((APPLIES,)),
            dma((APPLIES,)),
            dma((APPLIES,)),
            dma((APPLIES,)),
            dma((APPLIES,)),
            dma((APPLIES, n_bin)),
            dma((3,)),
            dma((3,)),
            dma((2, 3)),
            dma((2, 3)),
        ],
        compiler_params=pltpu.CompilerParams(collective_id=0, has_side_effects=True),
    )
    return call(
        start_factors,
        bin_factors.reshape(-1, tile, width),
        tile_speed[0, 0],
        tile_weight[0, 0],
        tile_cells[0, 0].T,
        tile_count,
        inner_pairs[0, 0],
        inner_weight[0, 0],
        face_rows[0, 0],
        face_count[0],
        face_weight[0, 0],
    )


def solution(mesh):
    lead = ("groups", "seg")
    rows = P(("groups", "seg", "bin"), None)
    in_specs = (
        rows,
        P(("groups", "bin"), None),
        P(lead, "bin", None, None, None),
        P(lead, "bin", None, None, None),
        P(lead, "bin", None, None),
        P(lead, "bin"),
        P(lead, "bin", None, None),
        P(lead, "bin", None, None, None),
        P(lead, "bin", None, None),
        P(lead, "bin", None),
        P(lead, "bin", None, None),
    )
    body = functools.partial(shards, mesh.shape["bin"], mesh.shape["seg"])
    return jax.shard_map(
        body, mesh=mesh, in_specs=in_specs, out_specs=(rows, rows), check_vma=False
    )
```

```python
import functools

import jax
import jax.numpy as jnp
from jax import lax
from jax.experimental import pallas as pl
from jax.experimental.pallas import tpu as pltpu
from jax.sharding import PartitionSpec as P

RIDGE = 0.5
APPLIES = 3
WAVES = 2
MESH = pl.DeviceIdType.MESH
f32 = jnp.float32
bf16 = jnp.bfloat16


def split(x):
    hi = x.astype(bf16)
    return hi, (x - hi.astype(f32)).astype(bf16)


def dot_nn(a, b):
    return jnp.dot(a, b, preferred_element_type=f32)


def dot_nt(a, b):
    return lax.dot_general(a, b, (((1,), (1,)), ((), ())), preferred_element_type=f32)


def kernel(
    n_bin,
    n_seg,
    x0_hbm,
    bins_hbm,
    speed_hbm,
    weight_hbm,
    cells_hbm,
    count_hbm,
    pairs_hbm,
    inner_hbm,
    rows_hbm,
    lives_hbm,
    face_hbm,
    sol_ref,
    res_ref,
    field,
    below,
    above,
    part,
    landed,
    halves,
    fulls,
    passed,
    summed,
    last,
    bins,
    speed,
    weight,
    cells,
    count,
    pairs,
    hits,
    inner,
    lives,
    listed,
    rows,
    rows_below,
    rows_above,
    face,
    face_above,
    gain,
    v_wide,
    v_tall,
    pulled,
    w_hi,
    w_lo,
    f_below,
    f_above,
    degree,
    rhs,
    base,
    whole,
    wide,
    sums_mine,
    sums_seg,
    sums_far,
    sums_all,
    sums_bin,
    load_sem,
    gather_send,
    gather_recv,
    below_send,
    below_recv,
    above_send,
    above_recv,
    scatter_send,
    scatter_recv,
    setup_send,
    setup_recv,
    sums_send,
    sums_recv,
):
    seg = lax.axis_index("seg")
    bin_ = lax.axis_index("bin")
    own = x0_hbm.shape[0]
    width = x0_hbm.shape[1]
    n_tiles = speed.shape[0]
    tile = speed.shape[1]
    n_inner = inner.shape[0]
    part_rows = own * n_bin
    n_blocks = part_rows // tile
    half = n_seg // 4
    seg_next = lax.rem(seg + 1, n_seg)
    seg_prev = lax.rem(seg + n_seg - 1, n_seg)

    def seg_at(offset):
        return lax.rem(seg + (offset + n_seg), n_seg)

    def bin_at(offset):
        return lax.rem(bin_ + offset, n_bin)

    def own_slice():
        return pl.ds(pl.multiple_of(bin_ * own, own), own)

    barrier = pltpu.get_barrier_semaphore()
    seg_offsets = [d for d in range(-half, half + 1) if d != 0]
    pairs_of = (
        (x0_hbm, field.at[0, own_slice()]),
        (rows_hbm, listed),
        (lives_hbm, lives),
        (face_hbm, face),
        (cells_hbm, cells),
        (count_hbm, count),
        (pairs_hbm, pairs),
        (bins_hbm, bins),
        (weight_hbm, weight),
        (speed_hbm, speed),
        (inner_hbm, inner),
    )
    loads = [pltpu.make_async_copy(src, dst, load_sem.at[at]) for at, (src, dst) in enumerate(pairs_of)]
    loads[0].start()
    for d in range(1, n_bin):
        pl.semaphore_signal(barrier, inc=1, device_id={"bin": bin_at(d)}, device_id_type=MESH)
    for d in seg_offsets:
        pl.semaphore_signal(barrier, inc=1, device_id={"seg": seg_at(d)}, device_id_type=MESH)
    for load in loads[1:]:
        load.start()

    def slots_and_gain():
        for load in loads[4:9]:
            load.wait()
        targets = [cells[0, k] for k in range(n_tiles)]
        targets += [pairs[j // 2, j % 2] for j in range(2 * n_inner)]
        for item, target in enumerate(targets):
            for b in range(n_blocks):
                away = target - b
                hits[item, b] = (1 - jnp.minimum(away * away, 1)).astype(f32)
        for k in range(n_tiles):
            live = jnp.clip(count[0, 0] - k, 0, 1).astype(f32)
            gain[k] = weight[k].astype(f32) * live
            chosen = bins[cells[1, k]]
            v_wide[k, :, :width] = chosen
            v_wide[k, :, width:] = chosen
            v_tall[k, :tile] = chosen
            v_tall[k, tile:] = chosen

    def add_up(items, block):
        total = None
        for ref_at, item in items:
            term = ref_at() * hits[item, block]
            total = term if total is None else total + term
        return total

    def right_side():
        loads[9].wait()
        for k in range(n_tiles):
            weighted = (weight[k].astype(f32) * speed[k].astype(f32)).astype(bf16)
            live = jnp.clip(count[0, 0] - k, 0, 1).astype(f32)
            pulled[k] = dot_nn(weighted, v_tall[k, :tile]) * live
        for b in range(n_blocks):
            items = [((lambda k=k: pulled[k]), k) for k in range(n_tiles)]
            rhs[b * tile : (b + 1) * tile] = add_up(items, b)

    def inner_setup():
        loads[10].wait()
        for j in range(n_inner):
            forward = inner[j]
            hi, lo = split(forward)
            w_hi[2 * j] = hi
            w_lo[2 * j] = lo
            back = forward.T
            hi, lo = split(back)
            w_hi[2 * j + 1] = hi
            w_lo[2 * j + 1] = lo
            pulled[2 * j] = jnp.broadcast_to(forward.sum(1, keepdims=True), (tile, width))
            pulled[2 * j + 1] = jnp.broadcast_to(back.sum(1, keepdims=True), (tile, width))

    def inner_degree(b):
        items = [((lambda j=j: pulled[j]), n_tiles + j) for j in range(2 * n_inner)]
        return add_up(items, b)

    def one_hot(row_ref, which):
        n_face = row_ref.shape[1]
        listed = jnp.broadcast_to(row_ref[which : which + 1, :], (part_rows, n_face))
        at = lax.broadcasted_iota(jnp.int32, (part_rows, n_face), 0)
        return jnp.where(listed == at, 1.0, 0.0).astype(bf16)

    def face_setup():
        low_own = one_hot(rows, 0)
        up_own = one_hot(rows, 1)
        up_below = one_hot(rows_below, 1)
        low_above = one_hot(rows_above, 0)
        down = jnp.where(seg > 0, 1.0, 0.0).astype(f32)
        up = jnp.where(seg < n_seg - 1, 1.0, 0.0).astype(f32)
        mine = split(face[...] * down)
        theirs = split(face_above[...] * up)
        degrees = jnp.zeros((part_rows, 1), f32)
        for p in range(2):
            picked = dot_nn(low_own, mine[p]).astype(bf16)
            whole = dot_nt(picked, up_below)
            f_below[p] = whole.astype(bf16)
            degrees = degrees + whole.sum(1, keepdims=True)
            picked = dot_nt(up_own, theirs[p]).astype(bf16)
            whole = dot_nt(picked, low_above)
            f_above[p] = whole.astype(bf16)
            degrees = degrees + whole.sum(1, keepdims=True)
        degree[...] = jnp.broadcast_to(degrees, (part_rows, width))
        for b in range(n_blocks):
            degree[b * tile : (b + 1) * tile] += inner_degree(b)

    def doubled(product):
        return product[:, :width] + product[:, width:]

    def local_terms(step):
        hi, lo = split(field[step])
        for b in range(n_blocks):
            wide[b, :, :width] = hi[b * tile : (b + 1) * tile]
            wide[b, :, width:] = lo[b * tile : (b + 1) * tile]
        for k in range(n_tiles):
            picked = wide[cells[0, k]]
            scores = dot_nt(picked, v_wide[k]) * gain[k]
            hi, lo = split(scores)
            pulled[k] = dot_nn(jnp.concatenate([hi, lo], axis=1), v_tall[k])
        for j in range(n_inner):
            for way in range(2):
                picked = wide[pairs[j, 1 - way]]
                product = doubled(dot_nn(w_hi[2 * j + way], picked))
                product = product + dot_nn(w_lo[2 * j + way], picked[:, :width])
                pulled[n_tiles + 2 * j + way] = -product

    def face_term(step, matrix, source):
        hi, lo = split(source[step])
        both = jnp.concatenate([hi, lo], axis=1)
        return doubled(dot_nn(matrix[0], both)) + dot_nn(matrix[1], hi)

    def base_terms(step):
        items = [((lambda k=k: pulled[k]), k) for k in range(n_tiles)]
        for j in range(2 * n_inner):
            items.append(((lambda j=j: pulled[n_tiles + j]), n_tiles + j))
        for b in range(n_blocks):
            at = slice(b * tile, (b + 1) * tile)
            value = add_up(items, b) + degree[at] * field[step, at]
            base[at] = value

    def join(step, faces):
        value = base[...] - faces
        part[step] = rhs[...] - value if step == 0 else value

    order = sorted(range(1, n_bin), key=lambda d: -min(d, n_bin - d))

    def to_bin(src, dst, send, recv, d):
        return pltpu.make_async_remote_copy(
            src_ref=src, dst_ref=dst, send_sem=send, recv_sem=recv,
            device_id={"bin": bin_at(d)}, device_id_type=MESH,
        )

    def to_seg(src, dst, send, recv, where):
        return pltpu.make_async_remote_copy(
            src_ref=src, dst_ref=dst, send_sem=send, recv_sem=recv,
            device_id={"seg": where}, device_id_type=MESH,
        )

    direct = lax.rem(seg, 2) == 0
    tree = jnp.logical_not(direct)
    slot_of = {-1: 0, 1: 1, -2: 2, 2: 3, -3: 4, 3: 5, -4: 6, 4: 7}
    straight = (4, 3, -3, 2, -2, 1, -1)
    wave_rows = own // WAVES

    def block_rows(wave, offset, part_of=None):
        at = lax.rem(bin_ + (offset + n_bin), n_bin) * own + wave * wave_rows
        size = wave_rows if part_of is None else wave_rows // 2
        if part_of:
            at = at + size
        return pl.ds(pl.multiple_of(at, size), size)

    def gather_send_to(step, wave, source, to, part_of=None):
        block = field.at[step, block_rows(wave, source, part_of)]
        recv = gather_recv.at[step, wave, slot_of[source - to]]
        to_bin(block, block, gather_send.at[step], recv, to + n_bin).start()

    def gather_take(step, wave, source, part_of=None):
        block = field.at[step, block_rows(wave, source, part_of)]
        pltpu.make_async_copy(block, block, gather_recv.at[step, wave, slot_of[source]]).wait()

    def pass_on(step, wave, source, part_of=None):
        rows_at = block_rows(wave, source, part_of)
        block = field.at[step, rows_at]
        to_seg(block, below.at[step, rows_at], below_send.at[step], below_recv.at[step], seg_next).start()
        to_seg(block, above.at[step, rows_at], above_send.at[step], above_recv.at[step], seg_prev).start()

    def gather_start(step, wave):
        @pl.when(direct)
        def _():
            for to in straight:
                gather_send_to(step, wave, 0, to)

        @pl.when(tree)
        def _():
            for to in (2, -2, 1, -1):
                gather_send_to(step, wave, 0, to)

        pass_on(step, wave, 0)

    def gather_relay(step):
        @pl.when(direct)
        def _():
            for source in (3, 2, -3, -2, 1, -1, -4):
                gather_take(step, 0, source)
                pass_on(step, 0, source)

        @pl.when(tree)
        def _():
            for wave in range(WAVES):
                for side in (-1, 1):
                    source = 2 * side
                    gather_take(step, wave, source)
                    gather_send_to(step, wave, source, -side)
                    gather_send_to(step, wave, source, -2 * side, 0 if side < 0 else 1)
                    pass_on(step, wave, source)
                for source in (-1, 1):
                    gather_take(step, wave, source)
                    pass_on(step, wave, source)

    def gather_finish(step):
        @pl.when(direct)
        def _():
            for wave in range(1, WAVES):
                for source in (3, 2, -3, -2, 1, -1, -4):
                    gather_take(step, wave, source)
                    pass_on(step, wave, source)

        @pl.when(tree)
        def _():
            for wave in range(WAVES):
                for source, part_of in ((-3, None), (3, None), (-4, 0), (4, 1)):
                    gather_take(step, wave, source, part_of)
                    pass_on(step, wave, source, part_of)

    def faces_join(step):
        def one(matrix, source, recv):
            pltpu.make_async_copy(source.at[step], source.at[step], recv.at[step]).wait()
            return face_term(step, matrix, source)

        @pl.when(direct)
        def _():
            base[...] -= one(f_above, above, above_recv)
            join(step, one(f_below, below, below_recv))

        @pl.when(tree)
        def _():
            base[...] -= one(f_below, below, below_recv)
            join(step, one(f_above, above, above_recv))

    def scatter_send_to(step, wave, src, dst, slot, to):
        to_bin(src, dst, scatter_send.at[step], scatter_recv.at[step, wave, slot], to + n_bin).start()

    def scatter_start(step):
        for wave in range(WAVES):
            @pl.when(direct)
            def _():
                for slot, to in enumerate(straight):
                    block = part.at[step, block_rows(wave, to)]
                    scatter_send_to(step, wave, block, landed.at[step, wave, slot], slot, to)

            @pl.when(tree)
            def _():
                for at, side in enumerate((-1, 1)):
                    far = part.at[step, block_rows(wave, 4, 1 - at)]
                    scatter_send_to(step, wave, far, halves.at[step, wave, at], 4 + at, 2 * side)
                    near = part.at[step, block_rows(wave, 3 * side)]
                    scatter_send_to(step, wave, near, fulls.at[step, wave, at], 6 + at, side)
                for at, side in enumerate((-1, 1)):
                    block = part.at[step, block_rows(wave, side)]
                    scatter_send_to(step, wave, block, landed.at[step, wave, at], at, side)

    def arrived(step, wave, ref, slot):
        pltpu.make_async_copy(ref, ref, scatter_recv.at[step, wave, slot]).wait()

    def scatter_relay(step):
        @pl.when(tree)
        def _():
            size = wave_rows // 2
            for wave in range(WAVES):
                for at, side in enumerate((-1, 1)):
                    arrived(step, wave, fulls.at[step, wave, at], 6 + at)
                    arrived(step, wave, halves.at[step, wave, at], 4 + at)
                    total = part[step, block_rows(wave, 2 * side)] + fulls[step, wave, at]
                    mine = slice((1 - at) * size, (2 - at) * size)
                    rest = slice(at * size, (at + 1) * size)
                    passed[step, wave, at, rest] = total[rest]
                    passed[step, wave, at, mine] = total[mine] + halves[step, wave, at]
                    dst = landed.at[step, wave, 2 + at]
                    scatter_send_to(step, wave, passed.at[step, wave, at], dst, 2 + at, 2 * side)

    def scatter_finish(step, wave):
        def add(slots):
            total = part[step, block_rows(wave, 0)]
            for slot in slots:
                arrived(step, wave, landed.at[step, wave, slot], slot)
                total = total + landed[step, wave, slot]
            summed[...] = total

        @pl.when(direct)
        def _():
            add(range(len(straight) - 1, -1, -1))

        @pl.when(tree)
        def _():
            add(range(4))

        return summed[...]

    window = [e for e in range(-half + 1, half + 1) if e != 0]

    def two_sums(first, second):
        lanes = lax.broadcasted_iota(jnp.int32, (1, width), 1)
        first = first.sum(0, keepdims=True)
        second = second.sum(0, keepdims=True)
        first = first + pltpu.roll(first, width // 2, 1)
        second = second + pltpu.roll(second, width // 2, 1)
        return jnp.where(lanes < width // 2, first, second)

    def sums_start(turn, value):
        sums_mine[turn, 0] = value
        for at, e in enumerate(window):
            to_seg(sums_mine.at[turn, 0], sums_seg.at[at], sums_send.at[turn, 0], sums_recv.at[turn, 0], seg_at(e)).start()

    def sums_second(turn):
        pltpu.make_async_copy(sums_seg, sums_seg, sums_recv.at[turn, 0]).wait()
        total = sums_mine[turn, 0]
        for at in range(len(window)):
            total = total + sums_seg[at]
        sums_mine[turn, 1] = total
        for at, e in enumerate((-half, half)):
            to_seg(sums_mine.at[turn, 1], sums_far.at[at], sums_send.at[turn, 1], sums_recv.at[turn, 1], seg_at(e)).start()

    def sums_third(turn):
        pltpu.make_async_copy(sums_far, sums_far, sums_recv.at[turn, 1]).wait()
        sums_to_bins(turn, sums_far[0] + sums_far[1])

    def sums_start_all(turn, value):
        sums_mine[turn, 0] = value
        for e in sorted(range(1, n_seg), key=lambda e: -min(e, n_seg - e)):
            to_seg(sums_mine.at[turn, 0], sums_all.at[e - 1], sums_send.at[turn, 0], sums_recv.at[turn, 0], seg_at(e)).start()

    def sums_third_all(turn):
        pltpu.make_async_copy(sums_all, sums_all, sums_recv.at[turn, 0]).wait()
        total = sums_mine[turn, 0]
        for e in range(1, n_seg):
            total = total + sums_all[e - 1]
        sums_to_bins(turn, total)

    def sums_to_bins(turn, total):
        sums_mine[turn, 2] = total
        for d in order:
            to_bin(sums_mine.at[turn, 2], sums_bin.at[turn, d - 1], sums_send.at[turn, 2], sums_recv.at[turn, 2], d).start()

    def sums_finish(turn):
        pltpu.make_async_copy(sums_bin.at[turn], sums_bin.at[turn], sums_recv.at[turn, 2]).wait()
        total = sums_mine[turn, 2]
        for d in range(n_bin - 1):
            total = total + sums_bin[turn, d]
        lanes = lax.broadcasted_iota(jnp.int32, (1, width), 1)
        first = jnp.sum(jnp.where(lanes < width // 2, total, 0.0), axis=1, keepdims=True)
        second = jnp.sum(jnp.where(lanes < width // 2, 0.0, total), axis=1, keepdims=True)
        return first, second

    loads[0].wait()
    pl.semaphore_wait(barrier, n_bin - 1 + len(seg_offsets))
    for wave in range(WAVES):
        gather_start(0, wave)
    for load in loads[1:3]:
        load.wait()
    slot_at = lax.broadcasted_iota(jnp.int32, (1, listed.shape[1]), 1)
    for side in range(2):
        own_list = listed[side : side + 1, :]
        rows[side : side + 1, :] = jnp.where(slot_at < lives[0, side], own_list, -1)
    loads[3].wait()
    to_seg(face, face_above, setup_send.at[2], setup_recv.at[2], seg_prev).start()
    to_seg(rows, rows_below, setup_send.at[0], setup_recv.at[0], seg_next).start()
    to_seg(rows, rows_above, setup_send.at[1], setup_recv.at[1], seg_prev).start()
    slots_and_gain()
    right_side()
    gather_relay(0)
    inner_setup()
    pltpu.make_async_copy(rows, rows_below, setup_recv.at[0]).wait()
    pltpu.make_async_copy(rows, rows_above, setup_recv.at[1]).wait()
    pltpu.make_async_copy(face, face_above, setup_recv.at[2]).wait()
    face_setup()
    gather_finish(0)
    local_terms(0)
    base_terms(0)
    faces_join(0)
    scatter_start(0)
    scatter_relay(0)
    for wave in range(WAVES):
        mine = block_rows(wave, 0)
        field[1, mine] = scatter_finish(0, wave) - RIDGE * field[0, mine]
        gather_start(1, wave)

    gather_relay(1)
    gather_finish(1)
    local_terms(1)
    base_terms(1)
    faces_join(1)
    residual = field[1, own_slice()]
    square = residual * residual
    scatter_start(1)
    sums_start(0, two_sums(square, field[1] * part[1]))
    scatter_relay(1)
    for wave in range(WAVES):
        mine = block_rows(wave, 0)
        field[2, mine] = scatter_finish(1, wave) + RIDGE * field[1, mine]
        gather_start(2, wave)
        if wave == 0:
            sums_second(0)
    gather_relay(2)
    sums_third(0)

    gather_finish(2)
    local_terms(2)
    base_terms(2)
    norm, product = sums_finish(0)
    product = product + RIDGE * norm
    step_one = norm / product
    residual = field[1, own_slice()]
    image = field[2, own_slice()]
    later = residual - step_one * image
    later_square = (later * later).sum(0, keepdims=True)
    whole[...] = field[1] - step_one * field[2]
    faces_join(2)
    whole_image = part[1] - step_one * part[2]
    sums_start_all(1, two_sums(later_square, whole[...] * whole_image))
    scatter_start(2)
    scatter_relay(2)
    sums_third_all(1)
    for wave in range(WAVES):
        mine = block_rows(wave, 0)
        last[wave * wave_rows : (wave + 1) * wave_rows] = scatter_finish(2, wave) + RIDGE * field[2, mine]
    norm_next, product_next = sums_finish(1)
    product_next = product_next + RIDGE * norm_next
    beta = norm_next / norm
    step_two = norm_next / (product_next - beta * norm_next / step_one)
    residual = field[1, own_slice()]
    image = field[2, own_slice()]
    later = residual - step_one * image
    later_image = image - step_one * last[...]
    direction = later + beta * residual
    along = later_image + beta * image
    sol_ref[...] = field[0, own_slice()] + step_one * residual + step_two * direction
    res_ref[...] = later - step_two * along

    pltpu.make_async_copy(rows, rows, setup_send.at[0]).wait()
    pltpu.make_async_copy(rows, rows, setup_send.at[1]).wait()
    pltpu.make_async_copy(face, face, setup_send.at[2]).wait()
    for step in range(APPLIES):
        sent = field.at[step, : (n_bin - 1) * own]
        pltpu.make_async_copy(sent, sent, gather_send.at[step]).wait()
        pltpu.make_async_copy(sent, sent, scatter_send.at[step]).wait()
        pltpu.make_async_copy(below.at[step], below.at[step], below_send.at[step]).wait()
        pltpu.make_async_copy(above.at[step], above.at[step], above_send.at[step]).wait()
    pltpu.make_async_copy(sums_seg, sums_seg, sums_send.at[0, 0]).wait()
    pltpu.make_async_copy(sums_far, sums_far, sums_send.at[0, 1]).wait()
    pltpu.make_async_copy(sums_all, sums_all, sums_send.at[1, 0]).wait()
    for turn in range(2):
        pltpu.make_async_copy(sums_bin.at[turn], sums_bin.at[turn], sums_send.at[turn, 2]).wait()


def finish_kernel(sol_in, res_in, sol_ref, res_ref):
    sol_ref[...] = sol_in[...]
    res_ref[...] = res_in[...]


def shards(
    n_bin,
    n_seg,
    start_factors,
    bin_factors,
    tile_speed,
    tile_weight,
    tile_cells,
    tile_count,
    inner_pairs,
    inner_weight,
    face_rows,
    face_count,
    face_weight,
):
    own, width = start_factors.shape
    n_tiles, tile = tile_speed.shape[2:4]
    n_inner = inner_weight.shape[2]
    n_face = face_rows.shape[3]
    part_rows = own * n_bin
    half = n_seg // 4
    window = 2 * half - 1
    any_ = pl.BlockSpec(memory_space=pl.ANY)
    vmem = pl.BlockSpec(memory_space=pltpu.VMEM)
    dma = pltpu.SemaphoreType.DMA
    call = pl.pallas_call(
        functools.partial(kernel, n_bin, n_seg),
        out_shape=(pltpu.VMEM((own, width), f32),) * 2,
        in_specs=[any_] * 11,
        out_specs=(vmem, vmem),
        scratch_shapes=[
            pltpu.VMEM((APPLIES, part_rows, width), f32),
            pltpu.VMEM((APPLIES, part_rows, width), f32),
            pltpu.VMEM((APPLIES, part_rows, width), f32),
            pltpu.VMEM((APPLIES, part_rows, width), f32),
            pltpu.VMEM((APPLIES, WAVES, 7, own // WAVES, width), f32),
            pltpu.VMEM((APPLIES, WAVES, 2, own // WAVES // 2, width), f32),
            pltpu.VMEM((APPLIES, WAVES, 2, own // WAVES, width), f32),
            pltpu.VMEM((APPLIES, WAVES, 2, own // WAVES, width), f32),
            pltpu.VMEM((own // WAVES, width), f32),
            pltpu.VMEM((own, width), f32),
            pltpu.VMEM((bin_factors.shape[0] // tile, tile, width), bf16),
            pltpu.VMEM((n_tiles, tile, tile), bf16),
            pltpu.VMEM((n_tiles, tile, tile), bf16),
            pltpu.SMEM((2, n_tiles), jnp.int32),
            pltpu.SMEM((1, 1), jnp.int32),
            pltpu.SMEM((n_inner, 2), jnp.int32),
            pltpu.SMEM((n_tiles + 2 * n_inner, part_rows // tile), f32),
            pltpu.VMEM((n_inner, tile, tile), f32),
            pltpu.SMEM((1, 2), jnp.int32),
            pltpu.VMEM((2, n_face), jnp.int32),
            pltpu.VMEM((2, n_face), jnp.int32),
            pltpu.VMEM((2, n_face), jnp.int32),
            pltpu.VMEM((2, n_face), jnp.int32),
            pltpu.VMEM((n_face, n_face), f32),
            pltpu.VMEM((n_face, n_face), f32),
            pltpu.VMEM((n_tiles, tile, tile), f32),
            pltpu.VMEM((n_tiles, tile, 2 * width), bf16),
            pltpu.VMEM((n_tiles, 2 * tile, width), bf16),
            pltpu.VMEM((n_tiles + 2 * n_inner, tile, width), f32),
            pltpu.VMEM((2 * n_inner, tile, tile), bf16),
            pltpu.VMEM((2 * n_inner, tile, tile), bf16),
            pltpu.VMEM((2, part_rows, part_rows), bf16),
            pltpu.VMEM((2, part_rows, part_rows), bf16),
            pltpu.VMEM((part_rows, width), f32),
            pltpu.VMEM((part_rows, width), f32),
            pltpu.VMEM((part_rows, width), f32),
            pltpu.VMEM((part_rows, width), f32),
            pltpu.VMEM((part_rows // tile, tile, 2 * width), bf16),
            pltpu.VMEM((2, 3, 1, width), f32),
            pltpu.VMEM((window, 1, width), f32),
            pltpu.VMEM((2, 1, width), f32),
            pltpu.VMEM((n_seg - 1, 1, width), f32),
            pltpu.VMEM((2, n_bin - 1, 1, width), f32),
            dma((11,)),
            dma((APPLIES,)),
            dma((APPLIES, WAVES, n_bin)),
            dma((APPLIES,)),
            dma((APPLIES,)),
            dma((APPLIES,)),
            dma((APPLIES,)),
            dma((APPLIES,)),
            dma((APPLIES, WAVES, n_bin)),
            dma((3,)),
            dma((3,)),
            dma((2, 3)),
            dma((2, 3)),
        ],
        compiler_params=pltpu.CompilerParams(collective_id=0, has_side_effects=True),
    )
    results = call(
        start_factors,
        bin_factors.reshape(-1, tile, width),
        tile_speed[0, 0],
        tile_weight[0, 0],
        tile_cells[0, 0].T,
        tile_count,
        inner_pairs[0, 0],
        inner_weight[0, 0],
        face_rows[0, 0],
        face_count[0],
        face_weight[0, 0],
    )
    held = [pltpu.with_memory_space_constraint(result, pltpu.VMEM) for result in results]
    out = jax.ShapeDtypeStruct((own, width), f32)
    finish = pl.pallas_call(
        finish_kernel, out_shape=(out, out), in_specs=[vmem] * 2, out_specs=(vmem, vmem)
    )
    return finish(*held)


def solution(mesh):
    lead = ("groups", "seg")
    rows = P(("groups", "seg", "bin"), None)
    in_specs = (
        rows,
        P(("groups", "bin"), None),
        P(lead, "bin", None, None, None),
        P(lead, "bin", None, None, None),
        P(lead, "bin", None, None),
        P(lead, "bin"),
        P(lead, "bin", None, None),
        P(lead, "bin", None, None, None),
        P(lead, "bin", None, None),
        P(lead, "bin", None),
        P(lead, "bin", None, None),
    )
    body = functools.partial(shards, mesh.shape["bin"], mesh.shape["seg"])
    return jax.shard_map(
        body, mesh=mesh, in_specs=in_specs, out_specs=(rows, rows), check_vma=False
    )
```

```python
import functools

import jax
import jax.numpy as jnp
from jax import lax
from jax.experimental import pallas as pl
from jax.experimental.pallas import tpu as pltpu
from jax.sharding import PartitionSpec as P

RIDGE = 0.5
APPLIES = 3
WAVES = 2
MESH = pl.DeviceIdType.MESH
f32 = jnp.float32
bf16 = jnp.bfloat16


def split(x):
    hi = x.astype(bf16)
    return hi, (x - hi.astype(f32)).astype(bf16)


def dot_nn(a, b):
    return jnp.dot(a, b, preferred_element_type=f32)


def dot_nt(a, b):
    return lax.dot_general(a, b, (((1,), (1,)), ((), ())), preferred_element_type=f32)


def kernel(
    n_bin,
    n_seg,
    x0_hbm,
    bins_hbm,
    speed_hbm,
    weight_hbm,
    cells_hbm,
    count_hbm,
    pairs_hbm,
    inner_hbm,
    rows_hbm,
    lives_hbm,
    face_hbm,
    sol_ref,
    res_ref,
    field,
    below,
    above,
    part,
    landed,
    halves,
    fulls,
    passed,
    summed,
    last,
    bins,
    speed,
    weight,
    cells,
    count,
    pairs,
    hits,
    inner,
    lives,
    listed,
    rows,
    rows_below,
    rows_above,
    face,
    face_above,
    gain,
    v_wide,
    v_tall,
    pulled,
    w_hi,
    w_lo,
    f_below,
    f_above,
    degree,
    rhs,
    base,
    whole,
    wide,
    sums_mine,
    sums_seg,
    sums_far,
    sums_all,
    sums_bin,
    load_sem,
    gather_send,
    gather_recv,
    below_send,
    below_recv,
    above_send,
    above_recv,
    scatter_send,
    scatter_recv,
    setup_send,
    setup_recv,
    sums_send,
    sums_recv,
):
    seg = lax.axis_index("seg")
    bin_ = lax.axis_index("bin")
    own = x0_hbm.shape[0]
    width = x0_hbm.shape[1]
    n_tiles = speed.shape[0]
    tile = speed.shape[1]
    n_inner = inner.shape[0]
    part_rows = own * n_bin
    n_blocks = part_rows // tile
    half = n_seg // 4
    seg_next = lax.rem(seg + 1, n_seg)
    seg_prev = lax.rem(seg + n_seg - 1, n_seg)

    def seg_at(offset):
        return lax.rem(seg + (offset + n_seg), n_seg)

    def bin_at(offset):
        return lax.rem(bin_ + offset, n_bin)

    def own_slice():
        return pl.ds(pl.multiple_of(bin_ * own, own), own)

    barrier = pltpu.get_barrier_semaphore()
    seg_offsets = [d for d in range(-half, half + 1) if d != 0]
    pairs_of = (
        (x0_hbm, field.at[0, own_slice()]),
        (rows_hbm, listed),
        (lives_hbm, lives),
        (face_hbm, face),
        (cells_hbm, cells),
        (count_hbm, count),
        (pairs_hbm, pairs),
        (bins_hbm, bins),
        (weight_hbm, weight),
        (speed_hbm, speed),
        (inner_hbm, inner),
    )
    loads = [pltpu.make_async_copy(src, dst, load_sem.at[at]) for at, (src, dst) in enumerate(pairs_of)]
    loads[0].start()
    for d in range(1, n_bin):
        pl.semaphore_signal(barrier, inc=1, device_id={"bin": bin_at(d)}, device_id_type=MESH)
    for d in seg_offsets:
        pl.semaphore_signal(barrier, inc=1, device_id={"seg": seg_at(d)}, device_id_type=MESH)
    for load in loads[1:]:
        load.start()

    def slots_and_gain():
        for load in loads[4:9]:
            load.wait()
        targets = [cells[0, k] for k in range(n_tiles)]
        targets += [pairs[j // 2, j % 2] for j in range(2 * n_inner)]
        for item, target in enumerate(targets):
            for b in range(n_blocks):
                away = target - b
                hits[item, b] = (1 - jnp.minimum(away * away, 1)).astype(f32)
        for k in range(n_tiles):
            live = jnp.clip(count[0, 0] - k, 0, 1).astype(f32)
            gain[k] = weight[k].astype(f32) * live
            chosen = bins[cells[1, k]]
            v_wide[k, :, :width] = chosen
            v_wide[k, :, width:] = chosen
            v_tall[k, :tile] = chosen
            v_tall[k, tile:] = chosen

    def add_up(items, block):
        total = None
        for ref_at, item in items:
            term = ref_at() * hits[item, block]
            total = term if total is None else total + term
        return total

    def right_side():
        loads[9].wait()
        for k in range(n_tiles):
            weighted = (weight[k].astype(f32) * speed[k].astype(f32)).astype(bf16)
            live = jnp.clip(count[0, 0] - k, 0, 1).astype(f32)
            pulled[k] = dot_nn(weighted, v_tall[k, :tile]) * live
        for b in range(n_blocks):
            items = [((lambda k=k: pulled[k]), k) for k in range(n_tiles)]
            rhs[b * tile : (b + 1) * tile] = add_up(items, b)

    def inner_setup():
        loads[10].wait()
        for j in range(n_inner):
            forward = inner[j]
            hi, lo = split(forward)
            w_hi[2 * j] = hi
            w_lo[2 * j] = lo
            back = forward.T
            hi, lo = split(back)
            w_hi[2 * j + 1] = hi
            w_lo[2 * j + 1] = lo
            pulled[2 * j] = jnp.broadcast_to(forward.sum(1, keepdims=True), (tile, width))
            pulled[2 * j + 1] = jnp.broadcast_to(back.sum(1, keepdims=True), (tile, width))

    def inner_degree(b):
        items = [((lambda j=j: pulled[j]), n_tiles + j) for j in range(2 * n_inner)]
        return add_up(items, b)

    def one_hot(row_ref, which):
        n_face = row_ref.shape[1]
        listed = jnp.broadcast_to(row_ref[which : which + 1, :], (part_rows, n_face))
        at = lax.broadcasted_iota(jnp.int32, (part_rows, n_face), 0)
        return jnp.where(listed == at, 1.0, 0.0).astype(bf16)

    def face_setup():
        low_own = one_hot(rows, 0)
        up_own = one_hot(rows, 1)
        up_below = one_hot(rows_below, 1)
        low_above = one_hot(rows_above, 0)
        down = jnp.where(seg > 0, 1.0, 0.0).astype(f32)
        up = jnp.where(seg < n_seg - 1, 1.0, 0.0).astype(f32)
        mine = split(face[...] * down)
        theirs = split(face_above[...] * up)
        degrees = jnp.zeros((part_rows, 1), f32)
        for p in range(2):
            picked = dot_nn(low_own, mine[p]).astype(bf16)
            whole = dot_nt(picked, up_below)
            f_below[p] = whole.astype(bf16)
            degrees = degrees + whole.sum(1, keepdims=True)
            picked = dot_nt(up_own, theirs[p]).astype(bf16)
            whole = dot_nt(picked, low_above)
            f_above[p] = whole.astype(bf16)
            degrees = degrees + whole.sum(1, keepdims=True)
        degree[...] = jnp.broadcast_to(degrees, (part_rows, width))
        for b in range(n_blocks):
            degree[b * tile : (b + 1) * tile] += inner_degree(b)

    def doubled(product):
        return product[:, :width] + product[:, width:]

    def local_terms(step):
        hi, lo = split(field[step])
        for b in range(n_blocks):
            wide[b, :, :width] = hi[b * tile : (b + 1) * tile]
            wide[b, :, width:] = lo[b * tile : (b + 1) * tile]
        for k in range(n_tiles):
            picked = wide[cells[0, k]]
            scores = dot_nt(picked, v_wide[k]) * gain[k]
            hi, lo = split(scores)
            pulled[k] = dot_nn(jnp.concatenate([hi, lo], axis=1), v_tall[k])
        for j in range(n_inner):
            for way in range(2):
                picked = wide[pairs[j, 1 - way]]
                product = doubled(dot_nn(w_hi[2 * j + way], picked))
                product = product + dot_nn(w_lo[2 * j + way], picked[:, :width])
                pulled[n_tiles + 2 * j + way] = -product

    def face_term(step, matrix, source):
        hi, lo = split(source[step])
        both = jnp.concatenate([hi, lo], axis=1)
        return doubled(dot_nn(matrix[0], both)) + dot_nn(matrix[1], hi)

    def base_terms(step):
        items = [((lambda k=k: pulled[k]), k) for k in range(n_tiles)]
        for j in range(2 * n_inner):
            items.append(((lambda j=j: pulled[n_tiles + j]), n_tiles + j))
        for b in range(n_blocks):
            at = slice(b * tile, (b + 1) * tile)
            value = add_up(items, b) + degree[at] * field[step, at]
            base[at] = value

    def join(step, faces):
        value = base[...] - faces
        part[step] = rhs[...] - value if step == 0 else value

    order = sorted(range(1, n_bin), key=lambda d: -min(d, n_bin - d))

    def to_bin(src, dst, send, recv, d):
        return pltpu.make_async_remote_copy(
            src_ref=src, dst_ref=dst, send_sem=send, recv_sem=recv,
            device_id={"bin": bin_at(d)}, device_id_type=MESH,
        )

    def to_seg(src, dst, send, recv, where):
        return pltpu.make_async_remote_copy(
            src_ref=src, dst_ref=dst, send_sem=send, recv_sem=recv,
            device_id={"seg": where}, device_id_type=MESH,
        )

    direct = lax.rem(seg, 2) == 0
    tree = jnp.logical_not(direct)
    slot_of = {-1: 0, 1: 1, -2: 2, 2: 3, -3: 4, 3: 5, -4: 6, 4: 7}
    straight = (4, 3, -3, 2, -2, 1, -1)
    wave_rows = own // WAVES

    def block_rows(wave, offset, part_of=None):
        at = lax.rem(bin_ + (offset + n_bin), n_bin) * own + wave * wave_rows
        size = wave_rows if part_of is None else wave_rows // 2
        if part_of:
            at = at + size
        return pl.ds(pl.multiple_of(at, size), size)

    def gather_send_to(step, wave, source, to, part_of=None):
        block = field.at[step, block_rows(wave, source, part_of)]
        recv = gather_recv.at[step, wave, slot_of[source - to]]
        to_bin(block, block, gather_send.at[step], recv, to + n_bin).start()

    def gather_take(step, wave, source, part_of=None):
        block = field.at[step, block_rows(wave, source, part_of)]
        pltpu.make_async_copy(block, block, gather_recv.at[step, wave, slot_of[source]]).wait()

    def pass_on(step, wave, source, part_of=None):
        rows_at = block_rows(wave, source, part_of)
        block = field.at[step, rows_at]
        to_seg(block, below.at[step, rows_at], below_send.at[step], below_recv.at[step], seg_next).start()
        to_seg(block, above.at[step, rows_at], above_send.at[step], above_recv.at[step], seg_prev).start()

    def gather_start(step, wave):
        @pl.when(direct)
        def _():
            for to in straight:
                gather_send_to(step, wave, 0, to)

        @pl.when(tree)
        def _():
            for to in (2, -2, 1, -1):
                gather_send_to(step, wave, 0, to)

        pass_on(step, wave, 0)

    def gather_relay(step):
        @pl.when(direct)
        def _():
            for source in (3, 2, -3, -2, 1, -1, -4):
                gather_take(step, 0, source)
                pass_on(step, 0, source)

        @pl.when(tree)
        def _():
            for wave in range(WAVES):
                for side in (-1, 1):
                    source = 2 * side
                    gather_take(step, wave, source)
                    gather_send_to(step, wave, source, -side)
                    gather_send_to(step, wave, source, -2 * side, 0 if side < 0 else 1)
                    pass_on(step, wave, source)
                for source in (-1, 1):
                    gather_take(step, wave, source)
                    pass_on(step, wave, source)

    def gather_finish(step):
        @pl.when(direct)
        def _():
            for wave in range(1, WAVES):
                for source in (3, 2, -3, -2, 1, -1, -4):
                    gather_take(step, wave, source)
                    pass_on(step, wave, source)

        @pl.when(tree)
        def _():
            for wave in range(WAVES):
                for source, part_of in ((-3, None), (3, None), (-4, 0), (4, 1)):
                    gather_take(step, wave, source, part_of)
                    pass_on(step, wave, source, part_of)

    def faces_join(step):
        def one(matrix, source, recv):
            pltpu.make_async_copy(source.at[step], source.at[step], recv.at[step]).wait()
            return face_term(step, matrix, source)

        @pl.when(direct)
        def _():
            base[...] -= one(f_above, above, above_recv)
            join(step, one(f_below, below, below_recv))

        @pl.when(tree)
        def _():
            base[...] -= one(f_below, below, below_recv)
            join(step, one(f_above, above, above_recv))

    def scatter_send_to(step, wave, src, dst, slot, to):
        to_bin(src, dst, scatter_send.at[step], scatter_recv.at[step, wave, slot], to + n_bin).start()

    def scatter_start(step):
        for wave in range(WAVES):
            @pl.when(direct)
            def _():
                for slot, to in enumerate(straight):
                    block = part.at[step, block_rows(wave, to)]
                    scatter_send_to(step, wave, block, landed.at[step, wave, slot], slot, to)

            @pl.when(tree)
            def _():
                for at, side in enumerate((-1, 1)):
                    far = part.at[step, block_rows(wave, 4, 1 - at)]
                    scatter_send_to(step, wave, far, halves.at[step, wave, at], 4 + at, 2 * side)
                    near = part.at[step, block_rows(wave, 3 * side)]
                    scatter_send_to(step, wave, near, fulls.at[step, wave, at], 6 + at, side)
                for at, side in enumerate((-1, 1)):
                    block = part.at[step, block_rows(wave, side)]
                    scatter_send_to(step, wave, block, landed.at[step, wave, at], at, side)

    def arrived(step, wave, ref, slot):
        pltpu.make_async_copy(ref, ref, scatter_recv.at[step, wave, slot]).wait()

    def scatter_relay(step):
        @pl.when(tree)
        def _():
            size = wave_rows // 2
            for wave in range(WAVES):
                for at, side in enumerate((-1, 1)):
                    arrived(step, wave, fulls.at[step, wave, at], 6 + at)
                    arrived(step, wave, halves.at[step, wave, at], 4 + at)
                    total = part[step, block_rows(wave, 2 * side)] + fulls[step, wave, at]
                    mine = slice((1 - at) * size, (2 - at) * size)
                    rest = slice(at * size, (at + 1) * size)
                    passed[step, wave, at, rest] = total[rest]
                    passed[step, wave, at, mine] = total[mine] + halves[step, wave, at]
                    dst = landed.at[step, wave, 2 + at]
                    scatter_send_to(step, wave, passed.at[step, wave, at], dst, 2 + at, 2 * side)

    def scatter_finish(step, wave):
        def add(slots):
            total = part[step, block_rows(wave, 0)]
            for slot in slots:
                arrived(step, wave, landed.at[step, wave, slot], slot)
                total = total + landed[step, wave, slot]
            summed[...] = total

        @pl.when(direct)
        def _():
            add(range(len(straight) - 1, -1, -1))

        @pl.when(tree)
        def _():
            add(range(4))

        return summed[...]

    window = [e for e in range(-half + 1, half + 1) if e != 0]

    def two_sums(first, second):
        lanes = lax.broadcasted_iota(jnp.int32, (1, width), 1)
        first = first.sum(0, keepdims=True)
        second = second.sum(0, keepdims=True)
        first = first + pltpu.roll(first, width // 2, 1)
        second = second + pltpu.roll(second, width // 2, 1)
        return jnp.where(lanes < width // 2, first, second)

    def sums_start(turn, value):
        sums_mine[turn, 0] = value
        for at, e in enumerate(window):
            to_seg(sums_mine.at[turn, 0], sums_seg.at[at], sums_send.at[turn, 0], sums_recv.at[turn, 0], seg_at(e)).start()

    def sums_second(turn):
        pltpu.make_async_copy(sums_seg, sums_seg, sums_recv.at[turn, 0]).wait()
        total = sums_mine[turn, 0]
        for at in range(len(window)):
            total = total + sums_seg[at]
        sums_mine[turn, 1] = total
        for at, e in enumerate((-half, half)):
            to_seg(sums_mine.at[turn, 1], sums_far.at[at], sums_send.at[turn, 1], sums_recv.at[turn, 1], seg_at(e)).start()

    def sums_third(turn):
        pltpu.make_async_copy(sums_far, sums_far, sums_recv.at[turn, 1]).wait()
        sums_to_bins(turn, sums_far[0] + sums_far[1])

    def sums_start_all(turn, value):
        sums_mine[turn, 0] = value
        for e in sorted(range(1, n_seg), key=lambda e: -min(e, n_seg - e)):
            to_seg(sums_mine.at[turn, 0], sums_all.at[e - 1], sums_send.at[turn, 0], sums_recv.at[turn, 0], seg_at(e)).start()

    def sums_third_all(turn):
        pltpu.make_async_copy(sums_all, sums_all, sums_recv.at[turn, 0]).wait()
        total = sums_mine[turn, 0]
        for e in range(1, n_seg):
            total = total + sums_all[e - 1]
        sums_to_bins(turn, total)

    def sums_to_bins(turn, total):
        sums_mine[turn, 2] = total
        for d in order:
            to_bin(sums_mine.at[turn, 2], sums_bin.at[turn, d - 1], sums_send.at[turn, 2], sums_recv.at[turn, 2], d).start()

    def sums_finish(turn):
        pltpu.make_async_copy(sums_bin.at[turn], sums_bin.at[turn], sums_recv.at[turn, 2]).wait()
        total = sums_mine[turn, 2]
        for d in range(n_bin - 1):
            total = total + sums_bin[turn, d]
        lanes = lax.broadcasted_iota(jnp.int32, (1, width), 1)
        first = jnp.sum(jnp.where(lanes < width // 2, total, 0.0), axis=1, keepdims=True)
        second = jnp.sum(jnp.where(lanes < width // 2, 0.0, total), axis=1, keepdims=True)
        return first, second

    loads[0].wait()
    pl.semaphore_wait(barrier, n_bin - 1 + len(seg_offsets))
    for wave in range(WAVES):
        gather_start(0, wave)
    for load in loads[1:3]:
        load.wait()
    slot_at = lax.broadcasted_iota(jnp.int32, (1, listed.shape[1]), 1)
    for side in range(2):
        own_list = listed[side : side + 1, :]
        rows[side : side + 1, :] = jnp.where(slot_at < lives[0, side], own_list, -1)
    loads[3].wait()
    to_seg(face, face_above, setup_send.at[2], setup_recv.at[2], seg_prev).start()
    to_seg(rows, rows_below, setup_send.at[0], setup_recv.at[0], seg_next).start()
    to_seg(rows, rows_above, setup_send.at[1], setup_recv.at[1], seg_prev).start()
    slots_and_gain()
    right_side()
    gather_relay(0)
    inner_setup()
    pltpu.make_async_copy(rows, rows_below, setup_recv.at[0]).wait()
    pltpu.make_async_copy(rows, rows_above, setup_recv.at[1]).wait()
    pltpu.make_async_copy(face, face_above, setup_recv.at[2]).wait()
    face_setup()
    gather_finish(0)
    local_terms(0)
    base_terms(0)
    faces_join(0)
    scatter_start(0)
    scatter_relay(0)
    for wave in range(WAVES):
        mine = block_rows(wave, 0)
        field[1, mine] = scatter_finish(0, wave) - RIDGE * field[0, mine]
        gather_start(1, wave)

    gather_relay(1)
    gather_finish(1)
    local_terms(1)
    base_terms(1)
    faces_join(1)
    residual = field[1, own_slice()]
    square = residual * residual
    scatter_start(1)
    sums_start(0, two_sums(square, field[1] * part[1]))
    scatter_relay(1)
    for wave in range(WAVES):
        mine = block_rows(wave, 0)
        field[2, mine] = scatter_finish(1, wave) + RIDGE * field[1, mine]
        gather_start(2, wave)
        if wave == 0:
            sums_second(0)
    gather_relay(2)
    sums_third(0)

    gather_finish(2)
    local_terms(2)
    base_terms(2)
    norm, product = sums_finish(0)
    product = product + RIDGE * norm
    step_one = norm / product
    residual = field[1, own_slice()]
    image = field[2, own_slice()]
    later = residual - step_one * image
    later_square = (later * later).sum(0, keepdims=True)
    whole[...] = field[1] - step_one * field[2]
    faces_join(2)
    whole_image = part[1] - step_one * part[2]
    sums_start_all(1, two_sums(later_square, whole[...] * whole_image))
    scatter_start(2)
    scatter_relay(2)
    sums_third_all(1)
    for wave in range(WAVES):
        mine = block_rows(wave, 0)
        last[wave * wave_rows : (wave + 1) * wave_rows] = scatter_finish(2, wave) + RIDGE * field[2, mine]
    residual = field[1, own_slice()]
    image = field[2, own_slice()]
    later = residual - step_one * image
    later_image = image - step_one * last[...]
    reached = field[0, own_slice()] + step_one * residual
    pltpu.make_async_copy(rows, rows, setup_send.at[0]).wait()
    pltpu.make_async_copy(rows, rows, setup_send.at[1]).wait()
    pltpu.make_async_copy(face, face, setup_send.at[2]).wait()
    for step in range(APPLIES):
        sent = field.at[step, : (n_bin - 1) * own]
        pltpu.make_async_copy(sent, sent, gather_send.at[step]).wait()
        pltpu.make_async_copy(sent, sent, scatter_send.at[step]).wait()
        pltpu.make_async_copy(below.at[step], below.at[step], below_send.at[step]).wait()
        pltpu.make_async_copy(above.at[step], above.at[step], above_send.at[step]).wait()
    pltpu.make_async_copy(sums_seg, sums_seg, sums_send.at[0, 0]).wait()
    pltpu.make_async_copy(sums_far, sums_far, sums_send.at[0, 1]).wait()
    pltpu.make_async_copy(sums_all, sums_all, sums_send.at[1, 0]).wait()
    pltpu.make_async_copy(sums_bin.at[0], sums_bin.at[0], sums_send.at[0, 2]).wait()
    pltpu.make_async_copy(sums_bin.at[1], sums_bin.at[1], sums_send.at[1, 2]).wait()
    norm_next, product_next = sums_finish(1)
    product_next = product_next + RIDGE * norm_next
    beta = norm_next / norm
    step_two = norm_next / (product_next - beta * norm_next / step_one)
    sol_ref[...] = reached + step_two * (later + beta * residual)
    res_ref[...] = later - step_two * (later_image + beta * image)


def finish_kernel(sol_in, res_in, sol_ref, res_ref):
    sol_ref[...] = sol_in[...]
    res_ref[...] = res_in[...]


def shards(
    n_bin,
    n_seg,
    start_factors,
    bin_factors,
    tile_speed,
    tile_weight,
    tile_cells,
    tile_count,
    inner_pairs,
    inner_weight,
    face_rows,
    face_count,
    face_weight,
):
    own, width = start_factors.shape
    n_tiles, tile = tile_speed.shape[2:4]
    n_inner = inner_weight.shape[2]
    n_face = face_rows.shape[3]
    part_rows = own * n_bin
    half = n_seg // 4
    window = 2 * half - 1
    any_ = pl.BlockSpec(memory_space=pl.ANY)
    vmem = pl.BlockSpec(memory_space=pltpu.VMEM)
    dma = pltpu.SemaphoreType.DMA
    call = pl.pallas_call(
        functools.partial(kernel, n_bin, n_seg),
        out_shape=(pltpu.VMEM((own, width), f32),) * 2,
        in_specs=[any_] * 11,
        out_specs=(vmem, vmem),
        scratch_shapes=[
            pltpu.VMEM((APPLIES, part_rows, width), f32),
            pltpu.VMEM((APPLIES, part_rows, width), f32),
            pltpu.VMEM((APPLIES, part_rows, width), f32),
            pltpu.VMEM((APPLIES, part_rows, width), f32),
            pltpu.VMEM((APPLIES, WAVES, 7, own // WAVES, width), f32),
            pltpu.VMEM((APPLIES, WAVES, 2, own // WAVES // 2, width), f32),
            pltpu.VMEM((APPLIES, WAVES, 2, own // WAVES, width), f32),
            pltpu.VMEM((APPLIES, WAVES, 2, own // WAVES, width), f32),
            pltpu.VMEM((own // WAVES, width), f32),
            pltpu.VMEM((own, width), f32),
            pltpu.VMEM((bin_factors.shape[0] // tile, tile, width), bf16),
            pltpu.VMEM((n_tiles, tile, tile), bf16),
            pltpu.VMEM((n_tiles, tile, tile), bf16),
            pltpu.SMEM((2, n_tiles), jnp.int32),
            pltpu.SMEM((1, 1), jnp.int32),
            pltpu.SMEM((n_inner, 2), jnp.int32),
            pltpu.SMEM((n_tiles + 2 * n_inner, part_rows // tile), f32),
            pltpu.VMEM((n_inner, tile, tile), f32),
            pltpu.SMEM((1, 2), jnp.int32),
            pltpu.VMEM((2, n_face), jnp.int32),
            pltpu.VMEM((2, n_face), jnp.int32),
            pltpu.VMEM((2, n_face), jnp.int32),
            pltpu.VMEM((2, n_face), jnp.int32),
            pltpu.VMEM((n_face, n_face), f32),
            pltpu.VMEM((n_face, n_face), f32),
            pltpu.VMEM((n_tiles, tile, tile), f32),
            pltpu.VMEM((n_tiles, tile, 2 * width), bf16),
            pltpu.VMEM((n_tiles, 2 * tile, width), bf16),
            pltpu.VMEM((n_tiles + 2 * n_inner, tile, width), f32),
            pltpu.VMEM((2 * n_inner, tile, tile), bf16),
            pltpu.VMEM((2 * n_inner, tile, tile), bf16),
            pltpu.VMEM((2, part_rows, part_rows), bf16),
            pltpu.VMEM((2, part_rows, part_rows), bf16),
            pltpu.VMEM((part_rows, width), f32),
            pltpu.VMEM((part_rows, width), f32),
            pltpu.VMEM((part_rows, width), f32),
            pltpu.VMEM((part_rows, width), f32),
            pltpu.VMEM((part_rows // tile, tile, 2 * width), bf16),
            pltpu.VMEM((2, 3, 1, width), f32),
            pltpu.VMEM((window, 1, width), f32),
            pltpu.VMEM((2, 1, width), f32),
            pltpu.VMEM((n_seg - 1, 1, width), f32),
            pltpu.VMEM((2, n_bin - 1, 1, width), f32),
            dma((11,)),
            dma((APPLIES,)),
            dma((APPLIES, WAVES, n_bin)),
            dma((APPLIES,)),
            dma((APPLIES,)),
            dma((APPLIES,)),
            dma((APPLIES,)),
            dma((APPLIES,)),
            dma((APPLIES, WAVES, n_bin)),
            dma((3,)),
            dma((3,)),
            dma((2, 3)),
            dma((2, 3)),
        ],
        compiler_params=pltpu.CompilerParams(collective_id=0, has_side_effects=True),
    )
    results = call(
        start_factors,
        bin_factors.reshape(-1, tile, width),
        tile_speed[0, 0],
        tile_weight[0, 0],
        tile_cells[0, 0].T,
        tile_count,
        inner_pairs[0, 0],
        inner_weight[0, 0],
        face_rows[0, 0],
        face_count[0],
        face_weight[0, 0],
    )
    held = [pltpu.with_memory_space_constraint(result, pltpu.VMEM) for result in results]
    out = jax.ShapeDtypeStruct((own, width), f32)
    finish = pl.pallas_call(
        finish_kernel, out_shape=(out, out), in_specs=[vmem] * 2, out_specs=(vmem, vmem)
    )
    return finish(*held)


def solution(mesh):
    lead = ("groups", "seg")
    rows = P(("groups", "seg", "bin"), None)
    in_specs = (
        rows,
        P(("groups", "bin"), None),
        P(lead, "bin", None, None, None),
        P(lead, "bin", None, None, None),
        P(lead, "bin", None, None),
        P(lead, "bin"),
        P(lead, "bin", None, None),
        P(lead, "bin", None, None, None),
        P(lead, "bin", None, None),
        P(lead, "bin", None),
        P(lead, "bin", None, None),
    )
    body = functools.partial(shards, mesh.shape["bin"], mesh.shape["seg"])
    return jax.shard_map(
        body, mesh=mesh, in_specs=in_specs, out_specs=(rows, rows), check_vma=False
    )
```
